32 devices in a mesh: seed: 4 (over x, core), train: 8 (over z, y).
Axes of the slice: x: 2, y: 2, z: 4, core: 2. Of those that a mesh axis runs over, the one named last changes fastest.
Arguments:
- coordinates: float32 [16, 524288], P('seed', 'train'), parts along dimension 0, may hold values from -6 to 6
- slice_index: int32 [2097152], P(('seed', 'train')), parts along dimension 0, may hold values from 0 to 127, as said below
- history: float32 [32, 2, 128, 1024], P('seed', None, None, 'train'), parts along dimension 0, may hold values from -3 to 3
- impedance: float32 [9, 2, 1024], replicated, may hold values from -1.2 to 1.2
- slice_wake: float32 [128, 128], replicated, may hold values from -0.5 to 0.5
- tunes: float32 [8], P('seed'), parts along dimension 0, may hold values from 0.05 to 0.45
- detuning: float32 [8], P('seed'), parts along dimension 0, may hold values from 0.1 to 0.4
Outputs:
- tracked: float32 [16, 524288], P('seed', 'train'), parts along dimension 0
- moments: float32 [8, 128, 1024], P('seed', None, 'train'), parts along dimension 0
The draws below stay inside these ranges and needn't reach their ends.
There are 4 independent parts, one for each index of `seed`. The reference program is written for one: setup_inputs(seed, part) draws one part's arguments, and reference() takes and returns one part's arrays. A program takes and returns all parts, laid end to end along the dimension named above; an argument that names none is the same for every part. Nothing has to cross between parts.
Inputs may be any that keep to these rules, and one draw needn't show every extreme that they name: `slice_index`: within each bunch, that is each aligned block of 512 entries, every slice number appears exactly 512 // 128 times.
All inputs are finite; a program needn't handle non-finite values.
Results may differ from the reference program's by a relative error of at most 0.00005.
Values sent between devices are 32-bit elements; how exact they have to be, the bound alone decides.
No kernel may reach another device: no remote copies, remote signals or barrier semaphores. Data moves between devices by JAX's collectives and lax.ppermute only.
A program may use at most 64 MiB of HBM per device.

```python
import math
import jax
import jax.numpy as jnp
from jax import lax

SLICES = 128
PARTICLES = 512
TURNS = 8
BUNCHES = 1024


def draw_slice_index(key, part):
    pattern = (jnp.arange(PARTICLES, dtype=jnp.int32) % SLICES).astype(jnp.int32)
    streams = jax.random.split(jax.random.fold_in(key, 7), BUNCHES)
    shuffled = jax.vmap(lambda stream: jax.random.permutation(stream, pattern))(streams)
    return shuffled.reshape(BUNCHES * PARTICLES).astype(jnp.int32)


def level_of(own_key, shape, cuts, low, top_value):
    def one(dim, parts):
        draws = jax.random.uniform(jax.random.fold_in(jax.random.fold_in(own_key, 6), dim), (parts,), jnp.float32, low / len(cuts), top_value / len(cuts))
        return jnp.repeat(jnp.exp(draws), shape[dim] // parts).reshape((-1,) + (1,) * (len(shape) - dim - 1))

    loudness = one(*cuts[0])
    for cut in cuts[1:]:
        loudness = loudness * one(*cut)
    return loudness


def scatter_about(key, extent, deviation, limit, cuts=(), kind=jnp.bfloat16):
    values = deviation * jax.random.normal(key, extent, jnp.float32)
    if cuts:
        values = values * level_of(key, extent, cuts, -0.22, 0.18)
    return jnp.clip(values, -limit, limit).astype(kind)


def setup_inputs(seed: int = 0, part: int = 0) -> dict:
    seeds = jax.random.split(jax.random.key(seed), 8)
    part_splits = jax.random.split(jax.random.fold_in(seeds[7], part), 8)
    coordinates = scatter_about(part_splits[0], (4, BUNCHES * PARTICLES), 1.0, 6.0, ((1, 8),), jnp.float32)
    slice_index = draw_slice_index(jax.random.fold_in(jax.random.fold_in(seeds[7], part), 71), part)
    history = scatter_about(part_splits[2], (TURNS, 2, SLICES, BUNCHES), 0.5, 3.0, ((3, 8),), jnp.float32)
    impedance = scatter_about(seeds[3], (TURNS + 1, 2, BUNCHES), 0.2, 1.2, (), jnp.float32)
    slice_wake = scatter_about(seeds[4], (SLICES, SLICES), SLICES ** -0.5, 0.5, (), jnp.float32)
    tunes = jnp.clip(jax.random.uniform(part_splits[5], (2,), jnp.float32, 0.05, 0.45), 0.05, 0.45)
    detuning = jnp.clip(jnp.exp(jax.random.uniform(part_splits[6], (2,), jnp.float32, math.log(0.1), math.log(0.4))), 0.1, 0.4)
    return {"coordinates": coordinates, "slice_index": slice_index, "history": history, "impedance": impedance, "slice_wake": slice_wake, "tunes": tunes, "detuning": detuning}


full_turn = 2.0 * math.pi


def rotate(positions, pushes, tunes, detuning):
    result = []
    for plane_index in range(2):
        position = positions[2 * plane_index]
        slope = positions[2 * plane_index + 1] + pushes[plane_index]
        action = 0.5 * (position * position + slope * slope)
        phase = full_turn * tunes[plane_index] + detuning[plane_index] * action
        cosine = jnp.cos(phase)
        sine = jnp.sin(phase)
        result.append(cosine * position + sine * slope)
        result.append(cosine * slope - sine * position)
    return jnp.stack(result)


def reference(coordinates, slice_index, history, impedance, slice_wake, tunes, detuning):
    owner = (lax.broadcasted_iota(jnp.int32, (BUNCHES * PARTICLES,), 0) // PARTICLES).astype(jnp.int32)
    segment = (slice_index * BUNCHES + owner).astype(jnp.int32)
    transverse = coordinates[0::2]
    sums = jax.vmap(lambda values: jax.ops.segment_sum(values, segment, num_segments=SLICES * BUNCHES))(transverse)
    moments = sums.reshape(2, SLICES, BUNCHES) * (SLICES / PARTICLES)
    series = jnp.concatenate([moments[None], history], 0)
    spectra = jnp.fft.fft(series, axis=-1)
    response = (impedance[:, 0] + 1j * impedance[:, 1])[:, None, None, :]
    summed = jnp.sum(response * spectra, axis=0)
    field = jnp.real(jnp.fft.ifft(summed, axis=-1))
    kicks = jnp.einsum("st,ctb->csb", slice_wake, field, precision=lax.Precision.HIGHEST)
    flat_kicks = kicks.reshape(2, SLICES * BUNCHES)
    pushes = jnp.take(flat_kicks, segment, axis=1)
    return rotate(coordinates, pushes, tunes, detuning), moments
```

```python
import math

import jax
import jax.numpy as jnp
import numpy as np
from jax import lax
from jax.experimental import pallas as pl
from jax.experimental.pallas import tpu as pltpu
from jax.sharding import PartitionSpec as P


full_turn = 2.0 * math.pi


def rotate(positions, pushes, tunes, detuning):
    result = []
    for plane_index in range(2):
        position = positions[2 * plane_index]
        slope = positions[2 * plane_index + 1] + pushes[plane_index]
        action = 0.5 * (position * position + slope * slope)
        phase = full_turn * tunes[plane_index] + detuning[plane_index] * action
        cosine = jnp.cos(phase)
        sine = jnp.sin(phase)
        result.append(cosine * position + sine * slope)
        result.append(cosine * slope - sine * position)
    return jnp.stack(result)


def phase_tables(row_count, col_count, period):
    first = lax.broadcasted_iota(jnp.int32, (row_count, col_count), 0)
    second = lax.broadcasted_iota(jnp.int32, (row_count, col_count), 1)
    angle = full_turn / period * (first * second % period).astype(jnp.float32)
    return (jnp.cos(angle), jnp.sin(angle))


def contract(form, table, values):
    return jnp.einsum(form, table, values, precision=lax.Precision.HIGHEST)


def forward(series):
    item_count, column_count, bunch_total = series.shape
    trains = lax.axis_size("train")
    bunch_dev = bunch_total // trains
    signal = series.reshape(item_count, column_count, trains, bunch_dev)
    cos_train, sin_train = phase_tables(trains, trains, trains)
    first_re = contract("kp,ncpj->nckj", cos_train, signal)
    first_im = -contract("kp,ncpj->nckj", sin_train, signal)
    cos_twist, sin_twist = phase_tables(trains, bunch_dev, bunch_total)
    twist_re = first_re * cos_twist + first_im * sin_twist
    twist_im = first_im * cos_twist - first_re * sin_twist
    cos_local, sin_local = phase_tables(bunch_dev, bunch_dev, bunch_dev)
    spec_re = contract("qj,nckj->ncqk", cos_local, twist_re) + contract(
        "qj,nckj->ncqk", sin_local, twist_im
    )
    spec_im = contract("qj,nckj->ncqk", cos_local, twist_im) - contract(
        "qj,nckj->ncqk", sin_local, twist_re
    )
    return (
        spec_re.reshape(item_count, column_count, bunch_total),
        spec_im.reshape(item_count, column_count, bunch_total),
    )


def inverse(summed_re, summed_im):
    column_count, bunch_total = summed_re.shape
    trains = lax.axis_size("train")
    bunch_dev = bunch_total // trains
    grid_re = summed_re.reshape(column_count, bunch_dev, trains)
    grid_im = summed_im.reshape(column_count, bunch_dev, trains)
    cos_local, sin_local = phase_tables(bunch_dev, bunch_dev, bunch_dev)
    back_re = contract("qj,cqk->ckj", cos_local, grid_re) - contract(
        "qj,cqk->ckj", sin_local, grid_im
    )
    back_im = contract("qj,cqk->ckj", cos_local, grid_im) + contract(
        "qj,cqk->ckj", sin_local, grid_re
    )
    cos_twist, sin_twist = phase_tables(trains, bunch_dev, bunch_total)
    turned_re = back_re * cos_twist - back_im * sin_twist
    turned_im = back_re * sin_twist + back_im * cos_twist
    cos_train, sin_train = phase_tables(trains, trains, trains)
    field = (
        contract("kp,ckj->cpj", cos_train, turned_re)
        - contract("kp,ckj->cpj", sin_train, turned_im)
    ) / bunch_total
    return field.reshape(column_count, bunch_total)


def generic(coordinates, slice_index, history, impedance, slice_wake, tunes, detuning):
    particle_count = slice_index.shape[0]
    slice_count = slice_wake.shape[0]
    bunch_dev = history.shape[3]
    turn_total = history.shape[0] + 1
    per_bunch = particle_count // bunch_dev
    bunch_group = math.gcd(bunch_dev, 16)
    group_count = bunch_dev // bunch_group
    group_span = bunch_group * per_bunch
    levels = lax.broadcasted_iota(jnp.int32, (1, 1, slice_count), 2)

    def selector(group_index):
        picked = lax.dynamic_slice_in_dim(slice_index, group_index * group_span, group_span)
        picked = picked.reshape(bunch_group, per_bunch)
        return (picked[:, :, None] == levels).astype(jnp.float32)

    def deposit(group_index, gathered):
        onehot = selector(group_index)
        section = lax.dynamic_slice_in_dim(coordinates, group_index * group_span, group_span, 1)
        transverse = section[0::2].reshape(2, bunch_group, per_bunch)
        sums = contract("gps,cgp->csg", onehot, transverse)
        return lax.dynamic_update_slice_in_dim(
            gathered, sums * (slice_count / per_bunch), group_index * bunch_group, 2
        )

    moments = lax.fori_loop(
        0, group_count, deposit, jnp.zeros((2, slice_count, bunch_dev), jnp.float32)
    )
    series = jnp.concatenate([moments[None], history], 0).reshape(
        turn_total, 2 * slice_count, bunch_dev
    )
    imp_re = impedance[:, 0, :]
    imp_im = impedance[:, 1, :]
    spec_re, spec_im = forward(
        lax.all_to_all(series, "train", split_axis=1, concat_axis=2, tiled=True)
    )
    summed_re = jnp.sum(imp_re[:, None, :] * spec_re - imp_im[:, None, :] * spec_im, axis=0)
    summed_im = jnp.sum(imp_re[:, None, :] * spec_im + imp_im[:, None, :] * spec_re, axis=0)
    field = inverse(summed_re, summed_im)
    home = lax.all_to_all(field, "train", split_axis=1, concat_axis=0, tiled=True).reshape(
        2, slice_count, bunch_dev
    )
    kicks = contract("st,ctb->csb", slice_wake, home)

    def track(group_index, moved):
        onehot = selector(group_index)
        local_kicks = lax.dynamic_slice_in_dim(kicks, group_index * bunch_group, bunch_group, 2)
        pushes = contract("gps,csg->cgp", onehot, local_kicks).reshape(2, group_span)
        section = lax.dynamic_slice_in_dim(coordinates, group_index * group_span, group_span, 1)
        turned = rotate(section, pushes, tunes, detuning)
        return lax.dynamic_update_slice_in_dim(moved, turned, group_index * group_span, 1)

    tracked = lax.fori_loop(0, group_count, track, jnp.zeros_like(coordinates))
    return (tracked, moments)


def split(values):
    high = values.astype(jnp.bfloat16)
    return high, (values - high.astype(jnp.float32)).astype(jnp.bfloat16)


def wide_dot(left, right):
    total = jnp.dot(left[0], right[0], preferred_element_type=jnp.float32)
    total += jnp.dot(left[0], right[1], preferred_element_type=jnp.float32)
    return total + jnp.dot(left[1], right[0], preferred_element_type=jnp.float32)


def wave_tables(trains, bunch_dev):
    total = trains * bunch_dev
    q = np.arange(bunch_dev)[:, None]
    n = np.arange(total)[None, :]
    angle = full_turn / total * (q * n % total)
    fine = np.concatenate([np.cos(angle), np.sin(angle)], 1)
    r = np.arange(trains)[:, None]
    lane = np.arange(bunch_dev)[None, :]
    coarse = full_turn / trains * (r * lane % trains)
    cosine, sine = np.cos(coarse) / total, np.sin(coarse) / total
    on_cos = np.stack([cosine, -sine], 1).reshape(2 * trains, bunch_dev)
    on_sin = np.stack([-sine, -cosine], 1).reshape(2 * trains, bunch_dev)
    return np.float32(fine), np.float32(np.stack([on_cos, on_sin]))


def front_kernel(
    odd_ref, coord_ref, index_ref, history_ref, impedance_ref, fine_ref, coarse_ref,
    moments_ref, keep0_ref, keep1_ref, send0_ref, send1_ref,
    high_ref, low_ref, xhigh_ref, xlow_ref, values_ref, places_ref,
):
    turns = history_ref.shape[0] + 1
    bunch_dev = history_ref.shape[2]
    total = high_ref.shape[1]
    trains = total // bunch_dev
    slices = moments_ref.shape[1]
    chunks = index_ref.shape[0] // bunch_dev

    waves = wide_dot(split(impedance_ref[...]), split(fine_ref[...]))
    on_cos = jnp.concatenate([coarse_ref[0]] * trains, 1)
    on_sin = jnp.concatenate([coarse_ref[1]] * trains, 1)
    for turn in range(turns):
        rows = waves[turn * 2 * trains : (turn + 1) * 2 * trains]
        kernel_row = jnp.sum(rows[:, :total] * on_cos + rows[:, total:] * on_sin, 0, keepdims=True)
        base = jnp.concatenate([pltpu.roll(kernel_row, i, 1) for i in range(16)], 0)
        for m in range(bunch_dev // 16):
            high, low = split(pltpu.roll(base, 16 * m, 1) if m else base)
            at = turn * bunch_dev + 16 * m
            high_ref[pl.ds(at, 16), :] = high
            low_ref[pl.ds(at, 16), :] = low

    for turn in range(1, turns):
        high, low = split(history_ref[turn - 1])
        xhigh_ref[:, turn * bunch_dev : (turn + 1) * bunch_dev] = high
        xlow_ref[:, turn * bunch_dev : (turn + 1) * bunch_dev] = low

    for chunk in range(chunks):
        at = pl.ds(chunk * 128, 128)
        places_ref[at, :] = index_ref[pl.ds(chunk, bunch_dev, stride=chunks), :].astype(jnp.float32).T
        for plane in range(2):
            start = 4 * chunk + 2 * plane
            values_ref[plane, at, :] = coord_ref[pl.ds(start, bunch_dev, stride=4 * chunks), :].T

    level = lax.broadcasted_iota(jnp.int32, (slices, bunch_dev), 0).astype(jnp.float32)

    def deposit(step, sums):
        first, second = sums
        for inner in range(8):
            at = pl.ds(step * 8 + inner, 1)
            hit = level == places_ref[at, :]
            first = first + jnp.where(hit, values_ref[0, at, :], 0.0)
            second = second + jnp.where(hit, values_ref[1, at, :], 0.0)
        return first, second

    zero = jnp.zeros((slices, bunch_dev), jnp.float32)
    sums = lax.fori_loop(0, chunks * 16, deposit, (zero, zero))
    for plane in range(2):
        current = sums[plane] * (slices / (chunks * 128))
        moments_ref[plane] = current
        high, low = split(current)
        xhigh_ref[pl.ds(plane * slices, slices), :bunch_dev] = high
        xlow_ref[pl.ds(plane * slices, slices), :bunch_dev] = low

    parity = odd_ref[0]
    half = trains // 2
    left = (xhigh_ref[...], xlow_ref[...])
    for block in range(half):
        at = pl.ds(2 * block * bunch_dev, 2 * bunch_dev)
        out = wide_dot(left, (high_ref[:, at], low_ref[:, at]))
        slot = lax.rem(block + parity, half)
        for plane, (keep_ref, send_ref) in enumerate(((keep0_ref, send0_ref), (keep1_ref, send1_ref))):
            part = out[plane * slices : (plane + 1) * slices]
            keep_ref[block] = part[:, :bunch_dev]
            send_ref[slot] = part[:, bunch_dev:]


def rotation(turn_quarters):
    whole = jnp.round(turn_quarters)
    rest = turn_quarters - whole
    square = rest * rest
    sine = rest * (1.5707963267948966 + square * (-0.6459640975062462 + square * (
        0.07969262624616703 + square * (-0.004681754135318687 + square * 0.00016044118478735982))))
    cosine = 1.0 + square * (-1.2337005501361697 + square * (0.253669507901048 + square * (
        -0.02086348076335296 + square * (0.0009192602748394264 + square * -0.000025202042373060603))))
    quadrant = whole.astype(jnp.int32)
    swap = (quadrant & 1) == 1
    cos_abs = jnp.where(swap, sine, cosine)
    sin_abs = jnp.where(swap, cosine, sine)
    cos_out = jnp.where(((quadrant + 1) & 2) == 2, -cos_abs, cos_abs)
    sin_out = jnp.where((quadrant & 2) == 2, -sin_abs, sin_abs)
    return cos_out, sin_out


def track_kernel(
    tunes_ref, detuning_ref, coord_ref, index_ref, wake_ref, *rest,
):
    part_refs, (moved_ref, kick_ref) = rest[:-2], rest[-2:]
    bunch_dev = wake_ref.shape[0]
    chunks = index_ref.shape[0] // bunch_dev
    wake = wake_ref[...]
    for plane in range(2):
        refs = part_refs[plane::2]
        field = refs[0][...]
        for ref in refs[1:]:
            field = field + ref[...]
        kick_ref[plane] = lax.dot_general(
            field.T, wake, (((1,), (1,)), ((), ())),
            precision=lax.Precision.HIGHEST, preferred_element_type=jnp.float32,
        )

    def group(step, carry):
        for chunk in range(chunks):
            picked = index_ref[pl.ds(step * 8 * chunks + chunk, 8, stride=chunks), :]
            for plane in range(2):
                start = step * 32 * chunks + 4 * chunk + 2 * plane
                at = pl.ds(start, 8, stride=4 * chunks)
                at_slope = pl.ds(start + 1, 8, stride=4 * chunks)
                table = kick_ref[plane, pl.ds(pl.multiple_of(step * 8, 8), 8), :]
                push = jnp.take_along_axis(table, picked, axis=1)
                position = coord_ref[at, :]
                slope = coord_ref[at_slope, :] + push
                square = position * position + slope * slope
                quarters = 4.0 * tunes_ref[plane] + (detuning_ref[plane] * (1.0 / math.pi)) * square
                cosine, sine = rotation(quarters)
                moved_ref[at, :] = cosine * position + sine * slope
                moved_ref[at_slope, :] = cosine * slope - sine * position
        return carry

    lax.fori_loop(0, bunch_dev // 8, group, 0)


def staged(coordinates, slice_index, history, impedance, slice_wake, tunes, detuning):
    turn_total, _, slice_count, bunch_dev = history.shape
    trains = lax.axis_size("train")
    bunch_total = trains * bunch_dev
    half = trains // 2
    lanes = 128
    columns = slice_index.shape[0] // lanes
    grid = coordinates.reshape(4, columns, lanes).transpose(1, 0, 2).reshape(4 * columns, lanes)
    picked = slice_index.reshape(columns, lanes)
    rows = impedance.reshape(turn_total + 1, 2, trains, bunch_dev).transpose(0, 2, 1, 3)
    rows = rows.reshape((turn_total + 1) * 2 * trains, bunch_dev)
    fine, coarse = wave_tables(trains, bunch_dev)
    odd = lax.rem(lax.axis_index("train"), 2).reshape(1)
    vmem = pl.BlockSpec(memory_space=pltpu.VMEM)
    smem = pl.BlockSpec(memory_space=pltpu.SMEM)
    block = jax.ShapeDtypeStruct((half, slice_count, bunch_dev), jnp.float32)
    depth = (turn_total + 1) * bunch_dev
    moments, keep0, keep1, send0, send1 = pl.pallas_call(
        front_kernel,
        out_shape=(jax.ShapeDtypeStruct((2, slice_count, bunch_dev), jnp.float32), block, block, block, block),
        in_specs=[smem] + [vmem] * 6,
        out_specs=[vmem] * 5,
        scratch_shapes=[
            pltpu.VMEM((depth, bunch_total), jnp.bfloat16),
            pltpu.VMEM((depth, bunch_total), jnp.bfloat16),
            pltpu.VMEM((2 * slice_count, depth), jnp.bfloat16),
            pltpu.VMEM((2 * slice_count, depth), jnp.bfloat16),
            pltpu.VMEM((2, columns * lanes // bunch_dev, bunch_dev), jnp.float32),
            pltpu.VMEM((columns * lanes // bunch_dev, bunch_dev), jnp.float32),
        ],
        name="front",
    )(odd, grid, picked, history.reshape(turn_total, 2 * slice_count, bunch_dev), rows, fine, coarse)

    pairs = [(i, i ^ 1) for i in range(trains)]
    parts = []
    for keep, send in ((keep0, send0), (keep1, send1)):
        near = keep + lax.ppermute(send, "train", pairs)
        mine = [near[0]]
        for hop in range(1, half):
            shift = [(i, (i + 2 * hop) % trains) for i in range(trains)]
            mine.append(lax.ppermute(near[hop], "train", shift))
        parts.append(mine)
    fields = [part for pair in zip(*parts) for part in pair]

    moved = pl.pallas_call(
        track_kernel,
        out_shape=jax.ShapeDtypeStruct(grid.shape, jnp.float32),
        in_specs=[smem, smem] + [vmem] * (3 + len(fields)),
        out_specs=vmem,
        scratch_shapes=[pltpu.VMEM((2, bunch_dev, slice_count), jnp.float32)],
        name="track",
    )(tunes, detuning, grid, picked, slice_wake, *fields)
    tracked = moved.reshape(columns, 4, lanes).transpose(1, 0, 2).reshape(4, columns * lanes)
    return (tracked, moments)


def local(coordinates, slice_index, history, impedance, slice_wake, tunes, detuning):
    trains = lax.axis_size("train")
    slice_count, bunch_dev = history.shape[2:]
    per_bunch = slice_index.shape[0] // bunch_dev
    fits = slice_count == bunch_dev == 128 and per_bunch % 128 == 0 and trains % 2 == 0 and trains <= 16
    body = staged if fits else generic
    return body(coordinates, slice_index, history, impedance, slice_wake, tunes, detuning)


def solution(mesh):
    return jax.shard_map(
        local,
        mesh=mesh,
        in_specs=(
            P("seed", "train"),
            P(("seed", "train")),
            P("seed", None, None, "train"),
            P(),
            P(),
            P("seed"),
            P("seed"),
        ),
        out_specs=(P("seed", "train"), P("seed", None, "train")),
        check_vma=False,
    )
```

```python
import math

import jax
import jax.numpy as jnp
import numpy as np
from jax import lax
from jax.experimental import pallas as pl
from jax.experimental.pallas import tpu as pltpu
from jax.sharding import PartitionSpec as P


full_turn = 2.0 * math.pi


def rotate(positions, pushes, tunes, detuning):
    result = []
    for plane_index in range(2):
        position = positions[2 * plane_index]
        slope = positions[2 * plane_index + 1] + pushes[plane_index]
        action = 0.5 * (position * position + slope * slope)
        phase = full_turn * tunes[plane_index] + detuning[plane_index] * action
        cosine = jnp.cos(phase)
        sine = jnp.sin(phase)
        result.append(cosine * position + sine * slope)
        result.append(cosine * slope - sine * position)
    return jnp.stack(result)


def phase_tables(row_count, col_count, period):
    first = lax.broadcasted_iota(jnp.int32, (row_count, col_count), 0)
    second = lax.broadcasted_iota(jnp.int32, (row_count, col_count), 1)
    angle = full_turn / period * (first * second % period).astype(jnp.float32)
    return (jnp.cos(angle), jnp.sin(angle))


def contract(form, table, values):
    return jnp.einsum(form, table, values, precision=lax.Precision.HIGHEST)


def forward(series):
    item_count, column_count, bunch_total = series.shape
    trains = lax.axis_size("train")
    bunch_dev = bunch_total // trains
    signal = series.reshape(item_count, column_count, trains, bunch_dev)
    cos_train, sin_train = phase_tables(trains, trains, trains)
    first_re = contract("kp,ncpj->nckj", cos_train, signal)
    first_im = -contract("kp,ncpj->nckj", sin_train, signal)
    cos_twist, sin_twist = phase_tables(trains, bunch_dev, bunch_total)
    twist_re = first_re * cos_twist + first_im * sin_twist
    twist_im = first_im * cos_twist - first_re * sin_twist
    cos_local, sin_local = phase_tables(bunch_dev, bunch_dev, bunch_dev)
    spec_re = contract("qj,nckj->ncqk", cos_local, twist_re) + contract(
        "qj,nckj->ncqk", sin_local, twist_im
    )
    spec_im = contract("qj,nckj->ncqk", cos_local, twist_im) - contract(
        "qj,nckj->ncqk", sin_local, twist_re
    )
    return (
        spec_re.reshape(item_count, column_count, bunch_total),
        spec_im.reshape(item_count, column_count, bunch_total),
    )


def inverse(summed_re, summed_im):
    column_count, bunch_total = summed_re.shape
    trains = lax.axis_size("train")
    bunch_dev = bunch_total // trains
    grid_re = summed_re.reshape(column_count, bunch_dev, trains)
    grid_im = summed_im.reshape(column_count, bunch_dev, trains)
    cos_local, sin_local = phase_tables(bunch_dev, bunch_dev, bunch_dev)
    back_re = contract("qj,cqk->ckj", cos_local, grid_re) - contract(
        "qj,cqk->ckj", sin_local, grid_im
    )
    back_im = contract("qj,cqk->ckj", cos_local, grid_im) + contract(
        "qj,cqk->ckj", sin_local, grid_re
    )
    cos_twist, sin_twist = phase_tables(trains, bunch_dev, bunch_total)
    turned_re = back_re * cos_twist - back_im * sin_twist
    turned_im = back_re * sin_twist + back_im * cos_twist
    cos_train, sin_train = phase_tables(trains, trains, trains)
    field = (
        contract("kp,ckj->cpj", cos_train, turned_re)
        - contract("kp,ckj->cpj", sin_train, turned_im)
    ) / bunch_total
    return field.reshape(column_count, bunch_total)


def generic(coordinates, slice_index, history, impedance, slice_wake, tunes, detuning):
    particle_count = slice_index.shape[0]
    slice_count = slice_wake.shape[0]
    bunch_dev = history.shape[3]
    turn_total = history.shape[0] + 1
    per_bunch = particle_count // bunch_dev
    bunch_group = math.gcd(bunch_dev, 16)
    group_count = bunch_dev // bunch_group
    group_span = bunch_group * per_bunch
    levels = lax.broadcasted_iota(jnp.int32, (1, 1, slice_count), 2)

    def selector(group_index):
        picked = lax.dynamic_slice_in_dim(slice_index, group_index * group_span, group_span)
        picked = picked.reshape(bunch_group, per_bunch)
        return (picked[:, :, None] == levels).astype(jnp.float32)

    def deposit(group_index, gathered):
        onehot = selector(group_index)
        section = lax.dynamic_slice_in_dim(coordinates, group_index * group_span, group_span, 1)
        transverse = section[0::2].reshape(2, bunch_group, per_bunch)
        sums = contract("gps,cgp->csg", onehot, transverse)
        return lax.dynamic_update_slice_in_dim(
            gathered, sums * (slice_count / per_bunch), group_index * bunch_group, 2
        )

    moments = lax.fori_loop(
        0, group_count, deposit, jnp.zeros((2, slice_count, bunch_dev), jnp.float32)
    )
    series = jnp.concatenate([moments[None], history], 0).reshape(
        turn_total, 2 * slice_count, bunch_dev
    )
    imp_re = impedance[:, 0, :]
    imp_im = impedance[:, 1, :]
    spec_re, spec_im = forward(
        lax.all_to_all(series, "train", split_axis=1, concat_axis=2, tiled=True)
    )
    summed_re = jnp.sum(imp_re[:, None, :] * spec_re - imp_im[:, None, :] * spec_im, axis=0)
    summed_im = jnp.sum(imp_re[:, None, :] * spec_im + imp_im[:, None, :] * spec_re, axis=0)
    field = inverse(summed_re, summed_im)
    home = lax.all_to_all(field, "train", split_axis=1, concat_axis=0, tiled=True).reshape(
        2, slice_count, bunch_dev
    )
    kicks = contract("st,ctb->csb", slice_wake, home)

    def track(group_index, moved):
        onehot = selector(group_index)
        local_kicks = lax.dynamic_slice_in_dim(kicks, group_index * bunch_group, bunch_group, 2)
        pushes = contract("gps,csg->cgp", onehot, local_kicks).reshape(2, group_span)
        section = lax.dynamic_slice_in_dim(coordinates, group_index * group_span, group_span, 1)
        turned = rotate(section, pushes, tunes, detuning)
        return lax.dynamic_update_slice_in_dim(moved, turned, group_index * group_span, 1)

    tracked = lax.fori_loop(0, group_count, track, jnp.zeros_like(coordinates))
    return (tracked, moments)


def split(values):
    high = values.astype(jnp.bfloat16)
    return high, (values - high.astype(jnp.float32)).astype(jnp.bfloat16)


def wide_dot(left, right):
    total = jnp.dot(left[0], right[0], preferred_element_type=jnp.float32)
    total += jnp.dot(left[0], right[1], preferred_element_type=jnp.float32)
    return total + jnp.dot(left[1], right[0], preferred_element_type=jnp.float32)


def wave_tables(trains, bunch_dev):
    total = trains * bunch_dev
    q = np.arange(bunch_dev)[:, None]
    n = np.arange(total)[None, :]
    angle = full_turn / total * (q * n % total)
    fine = np.float32(np.concatenate([np.cos(angle), np.sin(angle)], 1))
    fine_high = fine.astype(jnp.bfloat16)
    fine_low = (fine - fine_high.astype(np.float32)).astype(jnp.bfloat16)
    r = np.arange(trains)[:, None]
    lane = np.arange(bunch_dev)[None, :]
    coarse = full_turn / trains * (r * lane % trains)
    cosine, sine = np.cos(coarse) / total, np.sin(coarse) / total
    on_cos = np.stack([cosine, -sine], 1).reshape(2 * trains, bunch_dev)
    on_sin = np.stack([-sine, -cosine], 1).reshape(2 * trains, bunch_dev)
    return np.stack([fine_high, fine_low]), np.float32(np.stack([on_cos, on_sin]))


def swap_bits(blocks, lane):
    for step in (1, 2, 4):
        low = (lane & step) == 0
        for i in range(8):
            if not i & step:
                first, second = blocks[i], blocks[i | step]
                blocks[i] = jnp.where(low, first, pltpu.roll(second, step, 1))
                blocks[i | step] = jnp.where(low, pltpu.roll(first, 128 - step, 1), second)
    return blocks


def front_kernel(
    odd_ref, coord_hbm, index_hbm, history_hbm, impedance_ref, fine_ref, coarse_ref,
    moments_ref, keep0_ref, keep1_ref, send0_ref, send1_ref,
    high_ref, low_ref, xhigh_ref, xlow_ref, coord_ref, index_ref, history_ref, group_ref, waves_ref, sems,
):
    turns = history_ref.shape[0] + 1
    bunch_dev = history_ref.shape[2]
    total = high_ref.shape[1]
    trains = total // bunch_dev
    slices = moments_ref.shape[1]
    chunks = index_ref.shape[0] // bunch_dev
    copies = [
        pltpu.make_async_copy(source, target, sems.at[i])
        for i, (source, target) in enumerate(
            ((index_hbm, index_ref), (coord_hbm, coord_ref), (history_hbm, history_ref))
        )
    ]
    for copy in copies:
        copy.start()

    waves_ref[...] = wide_dot(split(impedance_ref[...]), (fine_ref[0], fine_ref[1]))
    row = lax.broadcasted_iota(jnp.int32, (8, bunch_dev), 0)
    lane = lax.broadcasted_iota(jnp.int32, (8, bunch_dev), 1)
    for turn in range(turns):
        rows = pl.ds(turn * 2 * trains, 2 * trains)
        pieces = []
        for block in range(trains):
            on_cos = waves_ref[rows, pl.ds(block * bunch_dev, bunch_dev)] * coarse_ref[0]
            on_sin = waves_ref[rows, pl.ds(total + block * bunch_dev, bunch_dev)] * coarse_ref[1]
            piece = jnp.sum(on_cos + on_sin, 0, keepdims=True)
            pieces.append(jnp.broadcast_to(piece, (8, bunch_dev)))
        for m in range(bunch_dev // 16):
            parts = []
            for shift in (16 * m, 16 * m + 8):
                inside = lane >= row + shift
                turned = [pltpu.roll(piece, shift, 1, stride=1, stride_axis=0) for piece in pieces]
                parts.append([jnp.where(inside, turned[d], turned[d - 1]) for d in range(trains)])
            at = turn * bunch_dev + 16 * m
            for d in range(trains):
                high, low = split(jnp.concatenate([parts[0][d], parts[1][d]], 0))
                high_ref[pl.ds(at, 16), pl.ds(d * bunch_dev, bunch_dev)] = high
                low_ref[pl.ds(at, 16), pl.ds(d * bunch_dev, bunch_dev)] = low

    copies[0].wait()
    copies[1].wait()
    digit = lax.broadcasted_iota(jnp.int32, (16, 128), 0)
    octal = lax.broadcasted_iota(jnp.int32, (8, 128), 0)

    def deposit(group, carry):
        placed = jnp.zeros((16, 128), jnp.float32)
        for inner in range(8):
            bunch = group * 8 + inner
            lows, values = [], []
            for chunk in range(chunks):
                place = index_ref[pl.ds(bunch * chunks + chunk, 1), :]
                lows.append(jnp.where(digit == (place & 15), 1.0, 0.0))
                hit = octal == (place >> 4)
                base = (bunch * chunks + chunk) * 4
                values.append(jnp.concatenate([
                    jnp.where(hit, coord_ref[pl.ds(base + 2 * plane, 1), :], 0.0) for plane in range(2)
                ], 0))
            onehot = jnp.concatenate(lows, 1).astype(jnp.bfloat16)
            both = jnp.concatenate(split(jnp.concatenate(values, 1)), 0)
            out = lax.dot_general(
                both, onehot, (((1,), (1,)), ((), ())), preferred_element_type=jnp.float32
            )
            out = jnp.concatenate([out[:16] + out[16:], jnp.zeros((16, 112), jnp.float32)], 1)
            placed = placed + (pltpu.roll(out, 16 * inner, 1) if inner else out)
        at = pl.ds(pl.multiple_of(group * 8, 8), 8)
        group_ref[0, at, :] = placed[:8]
        group_ref[1, at, :] = placed[8:]
        return carry

    lax.fori_loop(0, bunch_dev // 8, deposit, 0)
    lanes16 = lax.broadcasted_iota(jnp.int32, (16, 128), 1)
    for plane in range(2):
        turned = group_ref[plane].T
        blocks = swap_bits([turned[16 * i : 16 * i + 16] for i in range(8)], lanes16)
        current = jnp.concatenate(blocks, 0) * (slices / (chunks * 128))
        moments_ref[plane] = current
        high, low = split(current)
        xhigh_ref[pl.ds(plane * slices, slices), :bunch_dev] = high
        xlow_ref[pl.ds(plane * slices, slices), :bunch_dev] = low

    copies[2].wait()
    for turn in range(1, turns):
        high, low = split(history_ref[turn - 1])
        xhigh_ref[:, turn * bunch_dev : (turn + 1) * bunch_dev] = high
        xlow_ref[:, turn * bunch_dev : (turn + 1) * bunch_dev] = low

    parity = odd_ref[0]
    half = trains // 2
    left = (xhigh_ref[...], xlow_ref[...])
    for block in range(half):
        at = pl.ds(2 * block * bunch_dev, 2 * bunch_dev)
        out = wide_dot(left, (high_ref[:, at], low_ref[:, at]))
        slot = lax.rem(block + parity, half)
        for plane, (keep_ref, send_ref) in enumerate(((keep0_ref, send0_ref), (keep1_ref, send1_ref))):
            part = out[plane * slices : (plane + 1) * slices]
            keep_ref[block] = part[:, :bunch_dev]
            send_ref[slot] = part[:, bunch_dev:]


def rotation(turn_quarters):
    whole = jnp.round(turn_quarters)
    rest = turn_quarters - whole
    square = rest * rest
    sine = rest * (1.5707963267948966 + square * (-0.6459640975062462 + square * (
        0.07969262624616703 + square * (-0.004681754135318687 + square * 0.00016044118478735982))))
    cosine = 1.0 + square * (-1.2337005501361697 + square * (0.253669507901048 + square * (
        -0.02086348076335296 + square * (0.0009192602748394264 + square * -0.000025202042373060603))))
    quadrant = whole.astype(jnp.int32)
    swap = (quadrant & 1) == 1
    cos_abs = jnp.where(swap, sine, cosine)
    sin_abs = jnp.where(swap, cosine, sine)
    cos_out = jnp.where(((quadrant + 1) & 2) == 2, -cos_abs, cos_abs)
    sin_out = jnp.where((quadrant & 2) == 2, -sin_abs, sin_abs)
    return cos_out, sin_out


def track_kernel(
    tunes_ref, detuning_ref, coord_ref, index_ref, wake_ref, *rest,
):
    part_refs, (moved_hbm, kick_ref, moved_ref, sems) = rest[:-4], rest[-4:]
    bunch_dev = wake_ref.shape[0]
    chunks = index_ref.shape[0] // bunch_dev
    wake = split(wake_ref[...].T)
    for plane in range(2):
        refs = part_refs[plane::2]
        field = refs[0][...]
        for ref in refs[1:]:
            field = field + ref[...]
        kick_ref[plane] = wide_dot(split(field.T), wake)

    def group(step, carry):
        for chunk in range(chunks):
            picked = index_ref[pl.ds(step * 8 * chunks + chunk, 8, stride=chunks), :]
            for plane in range(2):
                start = step * 32 * chunks + 4 * chunk + 2 * plane
                at = pl.ds(start, 8, stride=4 * chunks)
                at_slope = pl.ds(start + 1, 8, stride=4 * chunks)
                table = kick_ref[plane, pl.ds(pl.multiple_of(step * 8, 8), 8), :]
                push = jnp.take_along_axis(table, picked, axis=1)
                position = coord_ref[at, :]
                slope = coord_ref[at_slope, :] + push
                square = position * position + slope * slope
                quarters = 4.0 * tunes_ref[plane] + (detuning_ref[plane] * (1.0 / math.pi)) * square
                cosine, sine = rotation(quarters)
                moved_ref[at, :] = cosine * position + sine * slope
                moved_ref[at_slope, :] = cosine * slope - sine * position
        return carry

    copies = []
    steps = bunch_dev // 8
    for piece in range(4):
        lax.fori_loop(piece * steps // 4, (piece + 1) * steps // 4, group, 0)
        span = pl.ds(piece * bunch_dev * chunks, bunch_dev * chunks)
        copies.append(pltpu.make_async_copy(moved_ref.at[span], moved_hbm.at[span], sems.at[piece]))
        copies[-1].start()
    for copy in copies:
        copy.wait()


def staged(coordinates, slice_index, history, impedance, slice_wake, tunes, detuning):
    turn_total, _, slice_count, bunch_dev = history.shape
    trains = lax.axis_size("train")
    bunch_total = trains * bunch_dev
    half = trains // 2
    lanes = 128
    columns = slice_index.shape[0] // lanes
    grid = coordinates.reshape(4, columns, lanes).transpose(1, 0, 2).reshape(4 * columns, lanes)
    picked = slice_index.reshape(columns, lanes)
    stacked = history.reshape(turn_total, 2 * slice_count, bunch_dev)
    rows = impedance.reshape(turn_total + 1, 2, trains, bunch_dev).transpose(0, 2, 1, 3)
    rows = rows.reshape((turn_total + 1) * 2 * trains, bunch_dev)
    fine, coarse = wave_tables(trains, bunch_dev)
    odd = lax.rem(lax.axis_index("train"), 2).reshape(1)
    vmem = pl.BlockSpec(memory_space=pltpu.VMEM)
    smem = pl.BlockSpec(memory_space=pltpu.SMEM)
    hbm = pl.BlockSpec(memory_space=pltpu.HBM)
    block = jax.ShapeDtypeStruct((half, slice_count, bunch_dev), jnp.float32)
    depth = (turn_total + 1) * bunch_dev
    moments, keep0, keep1, send0, send1 = pl.pallas_call(
        front_kernel,
        out_shape=(jax.ShapeDtypeStruct((2, slice_count, bunch_dev), jnp.float32), block, block, block, block),
        in_specs=[smem, hbm, hbm, hbm] + [vmem] * 3,
        out_specs=[vmem] * 5,
        scratch_shapes=[
            pltpu.VMEM((depth, bunch_total), jnp.bfloat16),
            pltpu.VMEM((depth, bunch_total), jnp.bfloat16),
            pltpu.VMEM((2 * slice_count, depth), jnp.bfloat16),
            pltpu.VMEM((2 * slice_count, depth), jnp.bfloat16),
            pltpu.VMEM(grid.shape, jnp.float32),
            pltpu.VMEM(picked.shape, jnp.int32),
            pltpu.VMEM(stacked.shape, jnp.float32),
            pltpu.VMEM((2, bunch_dev, slice_count), jnp.float32),
            pltpu.VMEM((rows.shape[0], 2 * bunch_total), jnp.float32),
            pltpu.SemaphoreType.DMA((3,)),
        ],
        compiler_params=pltpu.CompilerParams(vmem_limit_bytes=36 * 2**20),
        name="front",
    )(odd, grid, picked, stacked, rows, fine, coarse)

    pairs = [(i, i ^ 1) for i in range(trains)]
    parts = []
    for keep, send in ((keep0, send0), (keep1, send1)):
        far = lax.ppermute(send, "train", pairs)
        near = [keep[hop] + far[hop] for hop in range(half)]
        mine = [near[0]]
        for hop in range(1, half):
            shift = [(i, (i + 2 * hop) % trains) for i in range(trains)]
            mine.append(lax.ppermute(near[hop], "train", shift))
        parts.append(mine)
    fields = [part for pair in zip(*parts) for part in pair]

    moved = pl.pallas_call(
        track_kernel,
        out_shape=jax.ShapeDtypeStruct(grid.shape, jnp.float32),
        in_specs=[smem, smem] + [vmem] * (3 + len(fields)),
        out_specs=hbm,
        scratch_shapes=[
            pltpu.VMEM((2, bunch_dev, slice_count), jnp.float32),
            pltpu.VMEM(grid.shape, jnp.float32),
            pltpu.SemaphoreType.DMA((4,)),
        ],
        compiler_params=pltpu.CompilerParams(vmem_limit_bytes=16 * 2**20),
        name="track",
    )(tunes, detuning, grid, picked, slice_wake, *fields)
    tracked = moved.reshape(columns, 4, lanes).transpose(1, 0, 2).reshape(4, columns * lanes)
    return (tracked, moments)


def local(coordinates, slice_index, history, impedance, slice_wake, tunes, detuning):
    trains = lax.axis_size("train")
    slice_count, bunch_dev = history.shape[2:]
    per_bunch = slice_index.shape[0] // bunch_dev
    fits = slice_count == bunch_dev == 128 and per_bunch % 128 == 0 and trains % 2 == 0 and trains <= 16
    body = staged if fits else generic
    return body(coordinates, slice_index, history, impedance, slice_wake, tunes, detuning)


def solution(mesh):
    return jax.shard_map(
        local,
        mesh=mesh,
        in_specs=(
            P("seed", "train"),
            P(("seed", "train")),
            P("seed", None, None, "train"),
            P(),
            P(),
            P("seed"),
            P("seed"),
        ),
        out_specs=(P("seed", "train"), P("seed", None, "train")),
        check_vma=False,
    )
```

```python
import math

import jax
import jax.numpy as jnp
import numpy as np
from jax import lax
from jax.experimental import pallas as pl
from jax.experimental.pallas import tpu as pltpu
from jax.sharding import PartitionSpec as P


full_turn = 2.0 * math.pi


def rotate(positions, pushes, tunes, detuning):
    result = []
    for plane_index in range(2):
        position = positions[2 * plane_index]
        slope = positions[2 * plane_index + 1] + pushes[plane_index]
        action = 0.5 * (position * position + slope * slope)
        phase = full_turn * tunes[plane_index] + detuning[plane_index] * action
        cosine = jnp.cos(phase)
        sine = jnp.sin(phase)
        result.append(cosine * position + sine * slope)
        result.append(cosine * slope - sine * position)
    return jnp.stack(result)


def phase_tables(row_count, col_count, period):
    first = lax.broadcasted_iota(jnp.int32, (row_count, col_count), 0)
    second = lax.broadcasted_iota(jnp.int32, (row_count, col_count), 1)
    angle = full_turn / period * (first * second % period).astype(jnp.float32)
    return (jnp.cos(angle), jnp.sin(angle))


def contract(form, table, values):
    return jnp.einsum(form, table, values, precision=lax.Precision.HIGHEST)


def forward(series):
    item_count, column_count, bunch_total = series.shape
    trains = lax.axis_size("train")
    bunch_dev = bunch_total // trains
    signal = series.reshape(item_count, column_count, trains, bunch_dev)
    cos_train, sin_train = phase_tables(trains, trains, trains)
    first_re = contract("kp,ncpj->nckj", cos_train, signal)
    first_im = -contract("kp,ncpj->nckj", sin_train, signal)
    cos_twist, sin_twist = phase_tables(trains, bunch_dev, bunch_total)
    twist_re = first_re * cos_twist + first_im * sin_twist
    twist_im = first_im * cos_twist - first_re * sin_twist
    cos_local, sin_local = phase_tables(bunch_dev, bunch_dev, bunch_dev)
    spec_re = contract("qj,nckj->ncqk", cos_local, twist_re) + contract(
        "qj,nckj->ncqk", sin_local, twist_im
    )
    spec_im = contract("qj,nckj->ncqk", cos_local, twist_im) - contract(
        "qj,nckj->ncqk", sin_local, twist_re
    )
    return (
        spec_re.reshape(item_count, column_count, bunch_total),
        spec_im.reshape(item_count, column_count, bunch_total),
    )


def inverse(summed_re, summed_im):
    column_count, bunch_total = summed_re.shape
    trains = lax.axis_size("train")
    bunch_dev = bunch_total // trains
    grid_re = summed_re.reshape(column_count, bunch_dev, trains)
    grid_im = summed_im.reshape(column_count, bunch_dev, trains)
    cos_local, sin_local = phase_tables(bunch_dev, bunch_dev, bunch_dev)
    back_re = contract("qj,cqk->ckj", cos_local, grid_re) - contract(
        "qj,cqk->ckj", sin_local, grid_im
    )
    back_im = contract("qj,cqk->ckj", cos_local, grid_im) + contract(
        "qj,cqk->ckj", sin_local, grid_re
    )
    cos_twist, sin_twist = phase_tables(trains, bunch_dev, bunch_total)
    turned_re = back_re * cos_twist - back_im * sin_twist
    turned_im = back_re * sin_twist + back_im * cos_twist
    cos_train, sin_train = phase_tables(trains, trains, trains)
    field = (
        contract("kp,ckj->cpj", cos_train, turned_re)
        - contract("kp,ckj->cpj", sin_train, turned_im)
    ) / bunch_total
    return field.reshape(column_count, bunch_total)


def generic(coordinates, slice_index, history, impedance, slice_wake, tunes, detuning):
    particle_count = slice_index.shape[0]
    slice_count = slice_wake.shape[0]
    bunch_dev = history.shape[3]
    turn_total = history.shape[0] + 1
    per_bunch = particle_count // bunch_dev
    bunch_group = math.gcd(bunch_dev, 16)
    group_count = bunch_dev // bunch_group
    group_span = bunch_group * per_bunch
    levels = lax.broadcasted_iota(jnp.int32, (1, 1, slice_count), 2)

    def selector(group_index):
        picked = lax.dynamic_slice_in_dim(slice_index, group_index * group_span, group_span)
        picked = picked.reshape(bunch_group, per_bunch)
        return (picked[:, :, None] == levels).astype(jnp.float32)

    def deposit(group_index, gathered):
        onehot = selector(group_index)
        section = lax.dynamic_slice_in_dim(coordinates, group_index * group_span, group_span, 1)
        transverse = section[0::2].reshape(2, bunch_group, per_bunch)
        sums = contract("gps,cgp->csg", onehot, transverse)
        return lax.dynamic_update_slice_in_dim(
            gathered, sums * (slice_count / per_bunch), group_index * bunch_group, 2
        )

    moments = lax.fori_loop(
        0, group_count, deposit, jnp.zeros((2, slice_count, bunch_dev), jnp.float32)
    )
    series = jnp.concatenate([moments[None], history], 0).reshape(
        turn_total, 2 * slice_count, bunch_dev
    )
    imp_re = impedance[:, 0, :]
    imp_im = impedance[:, 1, :]
    spec_re, spec_im = forward(
        lax.all_to_all(series, "train", split_axis=1, concat_axis=2, tiled=True)
    )
    summed_re = jnp.sum(imp_re[:, None, :] * spec_re - imp_im[:, None, :] * spec_im, axis=0)
    summed_im = jnp.sum(imp_re[:, None, :] * spec_im + imp_im[:, None, :] * spec_re, axis=0)
    field = inverse(summed_re, summed_im)
    home = lax.all_to_all(field, "train", split_axis=1, concat_axis=0, tiled=True).reshape(
        2, slice_count, bunch_dev
    )
    kicks = contract("st,ctb->csb", slice_wake, home)

    def track(group_index, moved):
        onehot = selector(group_index)
        local_kicks = lax.dynamic_slice_in_dim(kicks, group_index * bunch_group, bunch_group, 2)
        pushes = contract("gps,csg->cgp", onehot, local_kicks).reshape(2, group_span)
        section = lax.dynamic_slice_in_dim(coordinates, group_index * group_span, group_span, 1)
        turned = rotate(section, pushes, tunes, detuning)
        return lax.dynamic_update_slice_in_dim(moved, turned, group_index * group_span, 1)

    tracked = lax.fori_loop(0, group_count, track, jnp.zeros_like(coordinates))
    return (tracked, moments)


def split(values):
    high = values.astype(jnp.bfloat16)
    return high, (values - high.astype(jnp.float32)).astype(jnp.bfloat16)


def wide_dot(left, right):
    total = jnp.dot(left[0], right[0], preferred_element_type=jnp.float32)
    total += jnp.dot(left[0], right[1], preferred_element_type=jnp.float32)
    return total + jnp.dot(left[1], right[0], preferred_element_type=jnp.float32)


def wave_table(trains, bunch_dev):
    total = trains * bunch_dev
    q = np.arange(bunch_dev)[:, None]
    n = np.arange(total)[None, :]
    angle = full_turn / total * (q * n % total)
    fine = np.float32(np.concatenate([np.cos(angle), np.sin(angle)], 1))
    fine_high = fine.astype(jnp.bfloat16)
    fine_low = (fine - fine_high.astype(np.float32)).astype(jnp.bfloat16)
    return np.stack([fine_high, fine_low])


def rotation(turn_quarters):
    whole = jnp.round(turn_quarters)
    rest = turn_quarters - whole
    square = rest * rest
    sine = rest * (1.5707963267948966 + square * (-0.6459640975062462 + square * (
        0.07969262624616703 + square * (-0.004681754135318687 + square * 0.00016044118478735982))))
    cosine = 1.0 + square * (-1.2337005501361697 + square * (0.253669507901048 + square * (
        -0.02086348076335296 + square * (0.0009192602748394264 + square * -0.000025202042373060603))))
    quadrant = whole.astype(jnp.int32)
    swap = (quadrant & 1) == 1
    cos_abs = jnp.where(swap, sine, cosine)
    sin_abs = jnp.where(swap, cosine, sine)
    cos_out = jnp.where(((quadrant + 1) & 2) == 2, -cos_abs, cos_abs)
    sin_out = jnp.where((quadrant & 2) == 2, -sin_abs, sin_abs)
    return cos_out, sin_out


def swap_bits(blocks, lane):
    for step in (1, 2, 4):
        low = (lane & step) == 0
        for i in range(8):
            if not i & step:
                first, second = blocks[i], blocks[i | step]
                blocks[i] = jnp.where(low, first, pltpu.roll(second, step, 1))
                blocks[i | step] = jnp.where(low, pltpu.roll(first, 128 - step, 1), second)
    return blocks


def front_kernel(
    odd_ref, coord_hbm, index_hbm, history_hbm, impedance_ref, fine_ref,
    moments_ref, keep0_ref, keep1_ref, send0_ref, send1_ref,
    high_ref, low_ref, xhigh_ref, xlow_ref, coord_ref, index_ref, history_ref, group_ref, waves_ref, sems,
):
    turns = history_ref.shape[0] + 1
    bunch_dev = history_ref.shape[2]
    total = high_ref.shape[1]
    trains = total // bunch_dev
    slices = moments_ref.shape[1]
    chunks = index_ref.shape[0] // bunch_dev
    copies = [
        pltpu.make_async_copy(source, target, sems.at[i])
        for i, (source, target) in enumerate(
            ((index_hbm, index_ref), (coord_hbm, coord_ref), (history_hbm, history_ref))
        )
    ]
    for copy in copies:
        copy.start()

    waves_ref[...] = wide_dot(split(impedance_ref[...]), (fine_ref[0], fine_ref[1]))
    row = lax.broadcasted_iota(jnp.int32, (8, bunch_dev), 0)
    lane = lax.broadcasted_iota(jnp.int32, (8, bunch_dev), 1)
    r = lax.broadcasted_iota(jnp.int32, (2 * trains, bunch_dev), 0)
    n = lax.broadcasted_iota(jnp.int32, (2 * trains, bunch_dev), 1)
    cosine, sine = rotation(lax.rem((r >> 1) * n, trains).astype(jnp.float32) * (4.0 / trains))
    real = (r & 1) == 0
    coarse_cos = jnp.where(real, cosine, -sine) * (1.0 / total)
    coarse_sin = jnp.where(real, -sine, -cosine) * (1.0 / total)
    for turn in range(turns):
        rows = pl.ds(turn * 2 * trains, 2 * trains)
        pieces = []
        for block in range(trains):
            on_cos = waves_ref[rows, pl.ds(block * bunch_dev, bunch_dev)] * coarse_cos
            on_sin = waves_ref[rows, pl.ds(total + block * bunch_dev, bunch_dev)] * coarse_sin
            piece = jnp.sum(on_cos + on_sin, 0, keepdims=True)
            pieces.append(jnp.broadcast_to(piece, (8, bunch_dev)))
        for m in range(bunch_dev // 16):
            parts = []
            for shift in (16 * m, 16 * m + 8):
                inside = lane >= row + shift
                turned = [pltpu.roll(piece, shift, 1, stride=1, stride_axis=0) for piece in pieces]
                parts.append([jnp.where(inside, turned[d], turned[d - 1]) for d in range(trains)])
            at = turn * bunch_dev + 16 * m
            for d in range(trains):
                high, low = split(jnp.concatenate([parts[0][d], parts[1][d]], 0))
                high_ref[pl.ds(at, 16), pl.ds(d * bunch_dev, bunch_dev)] = high
                low_ref[pl.ds(at, 16), pl.ds(d * bunch_dev, bunch_dev)] = low

    copies[0].wait()
    copies[1].wait()
    digit = lax.broadcasted_iota(jnp.int32, (16, 128), 0)
    octal = lax.broadcasted_iota(jnp.int32, (8, 128), 0)

    def deposit(group, carry):
        placed = jnp.zeros((16, 128), jnp.float32)
        for inner in range(8):
            bunch = group * 8 + inner
            lows, values = [], []
            for chunk in range(chunks):
                place = index_ref[pl.ds(bunch * chunks + chunk, 1), :]
                lows.append(jnp.where(digit == (place & 15), 1.0, 0.0))
                hit = octal == (place >> 4)
                base = (bunch * chunks + chunk) * 4
                values.append(jnp.concatenate([
                    jnp.where(hit, coord_ref[pl.ds(base + 2 * plane, 1), :], 0.0) for plane in range(2)
                ], 0))
            onehot = jnp.concatenate(lows, 1).astype(jnp.bfloat16)
            both = jnp.concatenate(split(jnp.concatenate(values, 1)), 0)
            out = lax.dot_general(
                both, onehot, (((1,), (1,)), ((), ())), preferred_element_type=jnp.float32
            )
            out = jnp.concatenate([out[:16] + out[16:], jnp.zeros((16, 112), jnp.float32)], 1)
            placed = placed + (pltpu.roll(out, 16 * inner, 1) if inner else out)
        at = pl.ds(pl.multiple_of(group * 8, 8), 8)
        group_ref[0, at, :] = placed[:8]
        group_ref[1, at, :] = placed[8:]
        return carry

    lax.fori_loop(0, bunch_dev // 8, deposit, 0)
    lanes16 = lax.broadcasted_iota(jnp.int32, (16, 128), 1)
    for plane in range(2):
        turned = group_ref[plane].T
        blocks = swap_bits([turned[16 * i : 16 * i + 16] for i in range(8)], lanes16)
        current = jnp.concatenate(blocks, 0) * (slices / (chunks * 128))
        moments_ref[plane] = current
        high, low = split(current)
        xhigh_ref[pl.ds(plane * slices, slices), :bunch_dev] = high
        xlow_ref[pl.ds(plane * slices, slices), :bunch_dev] = low

    copies[2].wait()
    for turn in range(1, turns):
        high, low = split(history_ref[turn - 1])
        xhigh_ref[:, turn * bunch_dev : (turn + 1) * bunch_dev] = high
        xlow_ref[:, turn * bunch_dev : (turn + 1) * bunch_dev] = low

    parity = odd_ref[0]
    half = trains // 2
    left = (xhigh_ref[...], xlow_ref[...])
    for block in range(half):
        at = pl.ds(2 * block * bunch_dev, 2 * bunch_dev)
        out = wide_dot(left, (high_ref[:, at], low_ref[:, at]))
        slot = lax.rem(block + parity, half)
        for plane, (keep_ref, send_ref) in enumerate(((keep0_ref, send0_ref), (keep1_ref, send1_ref))):
            part = out[plane * slices : (plane + 1) * slices]
            keep_ref[block] = part[:, :bunch_dev]
            send_ref[slot] = part[:, bunch_dev:]


def track_kernel(plane, coef_ref, coord_ref, index_ref, wake_ref, part_refs, kick_ref, store, finish):
    bunch_dev = wake_ref.shape[0]
    chunks = index_ref.shape[0] // bunch_dev
    field = part_refs[0][...]
    for ref in part_refs[1:]:
        field = field + ref[...]
    kick_ref[...] = wide_dot(split(field.T), split(wake_ref[...].T))
    tune, detune = coef_ref[plane], coef_ref[2 + plane]

    def group(step, carry):
        table = kick_ref[pl.ds(pl.multiple_of(step * 8, 8), 8), :]
        for chunk in range(chunks):
            picked = index_ref[pl.ds(step * 8 * chunks + chunk, 8, stride=chunks), :]
            start = step * 32 * chunks + 4 * chunk + 2 * plane
            push = jnp.take_along_axis(table, picked, axis=1)
            position = coord_ref[pl.ds(start, 8, stride=4 * chunks), :]
            slope = coord_ref[pl.ds(start + 1, 8, stride=4 * chunks), :] + push
            square = position * position + slope * slope
            cosine, sine = rotation(tune + detune * square)
            store(step, chunk, cosine * position + sine * slope, cosine * slope - sine * position)
        return carry

    steps = bunch_dev // 8
    for piece in range(4):
        lax.fori_loop(piece * steps // 4, (piece + 1) * steps // 4, group, 0)
        finish(piece)


def first_kernel(coef_ref, coord_ref, index_ref, wake_ref, *rest):
    part_refs, (moved_ref, kick_ref) = rest[:-2], rest[-2:]
    chunks = index_ref.shape[0] // wake_ref.shape[0]

    def store(step, chunk, position, slope):
        at = pl.ds(step * 8 * chunks + chunk, 8, stride=chunks)
        moved_ref[0, at, :] = position
        moved_ref[1, at, :] = slope

    track_kernel(0, coef_ref, coord_ref, index_ref, wake_ref, part_refs, kick_ref, store, lambda piece: None)


def second_kernel(coef_ref, coord_ref, index_ref, wake_ref, first_ref, *rest):
    part_refs, (moved_hbm, kick_ref, moved_ref, sems) = rest[:-4], rest[-4:]
    bunch_dev = wake_ref.shape[0]
    chunks = index_ref.shape[0] // bunch_dev
    copies = []

    def store(step, chunk, position, slope):
        start = step * 32 * chunks + 4 * chunk
        source = pl.ds(step * 8 * chunks + chunk, 8, stride=chunks)
        moved = (first_ref[0, source, :], first_ref[1, source, :], position, slope)
        for i in range(4):
            moved_ref[pl.ds(start + i, 8, stride=4 * chunks), :] = moved[i]

    def finish(piece):
        span = pl.ds(piece * bunch_dev * chunks, bunch_dev * chunks)
        copies.append(pltpu.make_async_copy(moved_ref.at[span], moved_hbm.at[span], sems.at[piece]))
        copies[-1].start()

    track_kernel(1, coef_ref, coord_ref, index_ref, wake_ref, part_refs, kick_ref, store, finish)
    for copy in copies:
        copy.wait()


def staged(coordinates, slice_index, history, impedance, slice_wake, tunes, detuning):
    turn_total, _, slice_count, bunch_dev = history.shape
    trains = lax.axis_size("train")
    bunch_total = trains * bunch_dev
    half = trains // 2
    lanes = 128
    columns = slice_index.shape[0] // lanes
    grid = coordinates.reshape(4, columns, lanes).transpose(1, 0, 2).reshape(4 * columns, lanes)
    picked = slice_index.reshape(columns, lanes)
    stacked = history.reshape(turn_total, 2 * slice_count, bunch_dev)
    rows = impedance.reshape(turn_total + 1, 2, trains, bunch_dev).transpose(0, 2, 1, 3)
    rows = rows.reshape((turn_total + 1) * 2 * trains, bunch_dev)
    fine = wave_table(trains, bunch_dev)
    odd = lax.rem(lax.axis_index("train"), 2).reshape(1)
    vmem = pl.BlockSpec(memory_space=pltpu.VMEM)
    smem = pl.BlockSpec(memory_space=pltpu.SMEM)
    hbm = pl.BlockSpec(memory_space=pltpu.HBM)
    block = jax.ShapeDtypeStruct((half, slice_count, bunch_dev), jnp.float32)
    depth = (turn_total + 1) * bunch_dev
    moments, keep0, keep1, send0, send1 = pl.pallas_call(
        front_kernel,
        out_shape=(jax.ShapeDtypeStruct((2, slice_count, bunch_dev), jnp.float32), block, block, block, block),
        in_specs=[smem, hbm, hbm, hbm] + [vmem] * 2,
        out_specs=[vmem] * 5,
        scratch_shapes=[
            pltpu.VMEM((depth, bunch_total), jnp.bfloat16),
            pltpu.VMEM((depth, bunch_total), jnp.bfloat16),
            pltpu.VMEM((2 * slice_count, depth), jnp.bfloat16),
            pltpu.VMEM((2 * slice_count, depth), jnp.bfloat16),
            pltpu.VMEM(grid.shape, jnp.float32),
            pltpu.VMEM(picked.shape, jnp.int32),
            pltpu.VMEM(stacked.shape, jnp.float32),
            pltpu.VMEM((2, bunch_dev, slice_count), jnp.float32),
            pltpu.VMEM((rows.shape[0], 2 * bunch_total), jnp.float32),
            pltpu.SemaphoreType.DMA((3,)),
        ],
        compiler_params=pltpu.CompilerParams(vmem_limit_bytes=54000 * 2**10),
        name="front",
    )(odd, grid, picked, stacked, rows, fine)

    pairs = [(i, i ^ 1) for i in range(trains)]
    parts = []
    for keep, send in ((keep0, send0), (keep1, send1)):
        far = lax.ppermute(send, "train", pairs)
        near = [keep[hop] + far[hop] for hop in range(half)]
        mine = [near[0]]
        for hop in range(1, half):
            shift = [(i, (i + 2 * hop) % trains) for i in range(trains)]
            mine.append(lax.ppermute(near[hop], "train", shift))
        parts.append(mine)
    marked = lax.optimization_barrier((tunes, detuning, parts[0][1]))
    coefs = jnp.concatenate([marked[0] * 4.0, marked[1] * (1.0 / math.pi)])
    parts[0][1] = marked[2]

    estimate = pl.CostEstimate(flops=2 * 10**9, transcendentals=0, bytes_accessed=10**6)
    first = pl.pallas_call(
        first_kernel,
        out_shape=jax.ShapeDtypeStruct((2,) + picked.shape, jnp.float32),
        in_specs=[smem] + [vmem] * (3 + half),
        out_specs=vmem,
        scratch_shapes=[pltpu.VMEM((bunch_dev, slice_count), jnp.float32)],
        compiler_params=pltpu.CompilerParams(vmem_limit_bytes=16 * 2**20),
        cost_estimate=estimate,
        name="first",
    )(coefs, grid, picked, slice_wake, *parts[0])
    moved = pl.pallas_call(
        second_kernel,
        out_shape=jax.ShapeDtypeStruct(grid.shape, jnp.float32),
        in_specs=[smem] + [vmem] * (4 + half),
        out_specs=hbm,
        scratch_shapes=[
            pltpu.VMEM((bunch_dev, slice_count), jnp.float32),
            pltpu.VMEM(grid.shape, jnp.float32),
            pltpu.SemaphoreType.DMA((4,)),
        ],
        compiler_params=pltpu.CompilerParams(vmem_limit_bytes=16 * 2**20),
        cost_estimate=estimate,
        name="second",
    )(coefs, grid, picked, slice_wake, first, *parts[1])
    tracked = moved.reshape(columns, 4, lanes).transpose(1, 0, 2).reshape(4, columns * lanes)
    return (tracked, moments)


def local(coordinates, slice_index, history, impedance, slice_wake, tunes, detuning):
    trains = lax.axis_size("train")
    slice_count, bunch_dev = history.shape[2:]
    per_bunch = slice_index.shape[0] // bunch_dev
    fits = slice_count == bunch_dev == 128 and per_bunch % 128 == 0 and trains % 2 == 0 and trains <= 16
    body = staged if fits else generic
    return body(coordinates, slice_index, history, impedance, slice_wake, tunes, detuning)


def solution(mesh):
    return jax.shard_map(
        local,
        mesh=mesh,
        in_specs=(
            P("seed", "train"),
            P(("seed", "train")),
            P("seed", None, None, "train"),
            P(),
            P(),
            P("seed"),
            P("seed"),
        ),
        out_specs=(P("seed", "train"), P("seed", None, "train")),
        check_vma=False,
    )
```

```python
import math

import jax
import jax.numpy as jnp
import numpy as np
from jax import lax
from jax.experimental import pallas as pl
from jax.experimental.pallas import tpu as pltpu
from jax.sharding import PartitionSpec as P


full_turn = 2.0 * math.pi


def rotate(positions, pushes, tunes, detuning):
    result = []
    for plane_index in range(2):
        position = positions[2 * plane_index]
        slope = positions[2 * plane_index + 1] + pushes[plane_index]
        action = 0.5 * (position * position + slope * slope)
        phase = full_turn * tunes[plane_index] + detuning[plane_index] * action
        cosine = jnp.cos(phase)
        sine = jnp.sin(phase)
        result.append(cosine * position + sine * slope)
        result.append(cosine * slope - sine * position)
    return jnp.stack(result)


def phase_tables(row_count, col_count, period):
    first = lax.broadcasted_iota(jnp.int32, (row_count, col_count), 0)
    second = lax.broadcasted_iota(jnp.int32, (row_count, col_count), 1)
    angle = full_turn / period * (first * second % period).astype(jnp.float32)
    return (jnp.cos(angle), jnp.sin(angle))


def contract(form, table, values):
    return jnp.einsum(form, table, values, precision=lax.Precision.HIGHEST)


def forward(series):
    item_count, column_count, bunch_total = series.shape
    trains = lax.axis_size("train")
    bunch_dev = bunch_total // trains
    signal = series.reshape(item_count, column_count, trains, bunch_dev)
    cos_train, sin_train = phase_tables(trains, trains, trains)
    first_re = contract("kp,ncpj->nckj", cos_train, signal)
    first_im = -contract("kp,ncpj->nckj", sin_train, signal)
    cos_twist, sin_twist = phase_tables(trains, bunch_dev, bunch_total)
    twist_re = first_re * cos_twist + first_im * sin_twist
    twist_im = first_im * cos_twist - first_re * sin_twist
    cos_local, sin_local = phase_tables(bunch_dev, bunch_dev, bunch_dev)
    spec_re = contract("qj,nckj->ncqk", cos_local, twist_re) + contract(
        "qj,nckj->ncqk", sin_local, twist_im
    )
    spec_im = contract("qj,nckj->ncqk", cos_local, twist_im) - contract(
        "qj,nckj->ncqk", sin_local, twist_re
    )
    return (
        spec_re.reshape(item_count, column_count, bunch_total),
        spec_im.reshape(item_count, column_count, bunch_total),
    )


def inverse(summed_re, summed_im):
    column_count, bunch_total = summed_re.shape
    trains = lax.axis_size("train")
    bunch_dev = bunch_total // trains
    grid_re = summed_re.reshape(column_count, bunch_dev, trains)
    grid_im = summed_im.reshape(column_count, bunch_dev, trains)
    cos_local, sin_local = phase_tables(bunch_dev, bunch_dev, bunch_dev)
    back_re = contract("qj,cqk->ckj", cos_local, grid_re) - contract(
        "qj,cqk->ckj", sin_local, grid_im
    )
    back_im = contract("qj,cqk->ckj", cos_local, grid_im) + contract(
        "qj,cqk->ckj", sin_local, grid_re
    )
    cos_twist, sin_twist = phase_tables(trains, bunch_dev, bunch_total)
    turned_re = back_re * cos_twist - back_im * sin_twist
    turned_im = back_re * sin_twist + back_im * cos_twist
    cos_train, sin_train = phase_tables(trains, trains, trains)
    field = (
        contract("kp,ckj->cpj", cos_train, turned_re)
        - contract("kp,ckj->cpj", sin_train, turned_im)
    ) / bunch_total
    return field.reshape(column_count, bunch_total)


def generic(coordinates, slice_index, history, impedance, slice_wake, tunes, detuning):
    particle_count = slice_index.shape[0]
    slice_count = slice_wake.shape[0]
    bunch_dev = history.shape[3]
    turn_total = history.shape[0] + 1
    per_bunch = particle_count // bunch_dev
    bunch_group = math.gcd(bunch_dev, 16)
    group_count = bunch_dev // bunch_group
    group_span = bunch_group * per_bunch
    levels = lax.broadcasted_iota(jnp.int32, (1, 1, slice_count), 2)

    def selector(group_index):
        picked = lax.dynamic_slice_in_dim(slice_index, group_index * group_span, group_span)
        picked = picked.reshape(bunch_group, per_bunch)
        return (picked[:, :, None] == levels).astype(jnp.float32)

    def deposit(group_index, gathered):
        onehot = selector(group_index)
        section = lax.dynamic_slice_in_dim(coordinates, group_index * group_span, group_span, 1)
        transverse = section[0::2].reshape(2, bunch_group, per_bunch)
        sums = contract("gps,cgp->csg", onehot, transverse)
        return lax.dynamic_update_slice_in_dim(
            gathered, sums * (slice_count / per_bunch), group_index * bunch_group, 2
        )

    moments = lax.fori_loop(
        0, group_count, deposit, jnp.zeros((2, slice_count, bunch_dev), jnp.float32)
    )
    series = jnp.concatenate([moments[None], history], 0).reshape(
        turn_total, 2 * slice_count, bunch_dev
    )
    imp_re = impedance[:, 0, :]
    imp_im = impedance[:, 1, :]
    spec_re, spec_im = forward(
        lax.all_to_all(series, "train", split_axis=1, concat_axis=2, tiled=True)
    )
    summed_re = jnp.sum(imp_re[:, None, :] * spec_re - imp_im[:, None, :] * spec_im, axis=0)
    summed_im = jnp.sum(imp_re[:, None, :] * spec_im + imp_im[:, None, :] * spec_re, axis=0)
    field = inverse(summed_re, summed_im)
    home = lax.all_to_all(field, "train", split_axis=1, concat_axis=0, tiled=True).reshape(
        2, slice_count, bunch_dev
    )
    kicks = contract("st,ctb->csb", slice_wake, home)

    def track(group_index, moved):
        onehot = selector(group_index)
        local_kicks = lax.dynamic_slice_in_dim(kicks, group_index * bunch_group, bunch_group, 2)
        pushes = contract("gps,csg->cgp", onehot, local_kicks).reshape(2, group_span)
        section = lax.dynamic_slice_in_dim(coordinates, group_index * group_span, group_span, 1)
        turned = rotate(section, pushes, tunes, detuning)
        return lax.dynamic_update_slice_in_dim(moved, turned, group_index * group_span, 1)

    tracked = lax.fori_loop(0, group_count, track, jnp.zeros_like(coordinates))
    return (tracked, moments)


def split(values):
    high = values.astype(jnp.bfloat16)
    return high, (values - high.astype(jnp.float32)).astype(jnp.bfloat16)


def wide_dot(left, right):
    total = jnp.dot(left[0], right[0], preferred_element_type=jnp.float32)
    total += jnp.dot(left[0], right[1], preferred_element_type=jnp.float32)
    return total + jnp.dot(left[1], right[0], preferred_element_type=jnp.float32)


def wave_table(trains, bunch_dev):
    total = trains * bunch_dev
    q = np.arange(bunch_dev)[:, None]
    n = np.arange(total)[None, :]
    angle = full_turn / total * (q * n % total)
    fine = np.float32(np.concatenate([np.cos(angle), np.sin(angle)], 1))
    fine_high = fine.astype(jnp.bfloat16)
    fine_low = (fine - fine_high.astype(np.float32)).astype(jnp.bfloat16)
    return np.stack([fine_high, fine_low])


def rotation(turn_quarters):
    whole = jnp.round(turn_quarters)
    rest = turn_quarters - whole
    square = rest * rest
    sine = rest * (1.5707963267948966 + square * (-0.6459640975062462 + square * (
        0.07969262624616703 + square * (-0.004681754135318687 + square * 0.00016044118478735982))))
    cosine = 1.0 + square * (-1.2337005501361697 + square * (0.253669507901048 + square * (
        -0.02086348076335296 + square * (0.0009192602748394264 + square * -0.000025202042373060603))))
    quadrant = whole.astype(jnp.int32)
    swap = (quadrant & 1) == 1
    cos_abs = jnp.where(swap, sine, cosine)
    sin_abs = jnp.where(swap, cosine, sine)
    cos_out = jnp.where(((quadrant + 1) & 2) == 2, -cos_abs, cos_abs)
    sin_out = jnp.where((quadrant & 2) == 2, -sin_abs, sin_abs)
    return cos_out, sin_out


def swap_bits(blocks, lane):
    for step in (1, 2, 4):
        low = (lane & step) == 0
        for i in range(8):
            if not i & step:
                first, second = blocks[i], blocks[i | step]
                blocks[i] = jnp.where(low, first, pltpu.roll(second, step, 1))
                blocks[i | step] = jnp.where(low, pltpu.roll(first, 128 - step, 1), second)
    return blocks


def front_kernel(
    odd_ref, coord_hbm, index_hbm, history_hbm, impedance_hbm, fine_hbm,
    moments_hbm, keep0_ref, keep1_ref, send0_ref, send1_ref,
    moments_ref, high_ref, low_ref, xhigh_ref, xlow_ref, coord_ref, index_ref, history_ref, group_ref, waves_ref, impedance_ref, fine_ref, sems,
):
    turns = history_ref.shape[0] + 1
    bunch_dev = history_ref.shape[2]
    total = high_ref.shape[1]
    trains = total // bunch_dev
    slices = moments_ref.shape[1]
    chunks = index_ref.shape[0] // bunch_dev
    copies = [
        pltpu.make_async_copy(source, target, sems.at[i])
        for i, (source, target) in enumerate(
            ((impedance_hbm, impedance_ref), (fine_hbm, fine_ref), (index_hbm, index_ref), (coord_hbm, coord_ref),
             (history_hbm, history_ref))
        )
    ]
    for copy in copies:
        copy.start()

    copies[0].wait()
    copies[1].wait()
    high, low = split(impedance_ref[...])

    def wave(block, carry):
        at = pl.ds(pl.multiple_of(block * 256, 256), 256)
        waves_ref[:, at] = wide_dot((high, low), (fine_ref[0, :, at], fine_ref[1, :, at]))
        return carry

    for block in range(2 * total // 256):
        wave(block, 0)
    row = lax.broadcasted_iota(jnp.int32, (8, bunch_dev), 0)
    lane = lax.broadcasted_iota(jnp.int32, (8, bunch_dev), 1)
    r = lax.broadcasted_iota(jnp.int32, (2 * trains, bunch_dev), 0)
    n = lax.broadcasted_iota(jnp.int32, (2 * trains, bunch_dev), 1)
    cosine, sine = rotation(lax.rem((r >> 1) * n, trains).astype(jnp.float32) * (4.0 / trains))
    real = (r & 1) == 0
    coarse_cos = jnp.where(real, cosine, -sine) * (1.0 / total)
    coarse_sin = jnp.where(real, -sine, -cosine) * (1.0 / total)
    def circulant(turn, carry):
        rows = pl.ds(pl.multiple_of(turn * 2 * trains, 2 * trains), 2 * trains)
        pieces = []
        for block in range(trains):
            on_cos = waves_ref[rows, pl.ds(block * bunch_dev, bunch_dev)] * coarse_cos
            on_sin = waves_ref[rows, pl.ds(total + block * bunch_dev, bunch_dev)] * coarse_sin
            piece = jnp.sum(on_cos + on_sin, 0, keepdims=True)
            pieces.append(jnp.broadcast_to(piece, (8, bunch_dev)))
        for m in range(bunch_dev // 16):
            parts = []
            for shift in (16 * m, 16 * m + 8):
                inside = lane >= row + shift
                turned = [pltpu.roll(piece, shift, 1, stride=1, stride_axis=0) for piece in pieces]
                parts.append([jnp.where(inside, turned[d], turned[d - 1]) for d in range(trains)])
            at = pl.multiple_of(turn * bunch_dev + 16 * m, 16)
            for d in range(trains):
                high, low = split(jnp.concatenate([parts[0][d], parts[1][d]], 0))
                high_ref[pl.ds(at, 16), pl.ds(d * bunch_dev, bunch_dev)] = high
                low_ref[pl.ds(at, 16), pl.ds(d * bunch_dev, bunch_dev)] = low
        return carry

    for turn in range(turns):
        circulant(turn, 0)
    copies[2].wait()
    copies[3].wait()
    digit = lax.broadcasted_iota(jnp.int32, (16, 128), 0)
    octal = lax.broadcasted_iota(jnp.int32, (8, 128), 0)

    owner = lax.broadcasted_iota(jnp.int32, (16, 128), 1) >> 4

    def deposit(group, carry):
        lows, values = [], []
        for inner in range(8):
            bunch = group * 8 + inner
            low_rows, value_rows = [], []
            for chunk in range(chunks):
                place = index_ref[pl.ds(bunch * chunks + chunk, 1), :]
                low_rows.append(jnp.where(digit == (place & 15), 1.0, 0.0))
                hit = octal == (place >> 4)
                base = (bunch * chunks + chunk) * 4
                value_rows.append(jnp.concatenate([
                    jnp.where(hit, coord_ref[pl.ds(base + 2 * plane, 1), :], 0.0) for plane in range(2)
                ], 0))
            lows.append(jnp.concatenate(low_rows, 1).astype(jnp.bfloat16))
            values.append(jnp.concatenate(value_rows, 1))
        both = jnp.concatenate(split(jnp.concatenate(values, 0)), 0)
        out = lax.dot_general(
            both, jnp.concatenate(lows, 0), (((1,), (1,)), ((), ())), preferred_element_type=jnp.float32
        )
        placed = jnp.zeros((16, 128), jnp.float32)
        for inner in range(8):
            at = 16 * inner
            placed = jnp.where(owner == inner, out[at : at + 16] + out[128 + at : 144 + at], placed)
        at = pl.ds(pl.multiple_of(group * 8, 8), 8)
        group_ref[0, at, :] = placed[:8]
        group_ref[1, at, :] = placed[8:]
        return carry

    lax.fori_loop(0, bunch_dev // 8, deposit, 0, unroll=16)
    lanes16 = lax.broadcasted_iota(jnp.int32, (16, 128), 1)
    for plane in range(2):
        turned = group_ref[plane].T
        blocks = swap_bits([turned[16 * i : 16 * i + 16] for i in range(8)], lanes16)
        current = jnp.concatenate(blocks, 0) * (slices / (chunks * 128))
        moments_ref[plane] = current
        high, low = split(current)
        xhigh_ref[pl.ds(plane * slices, slices), :bunch_dev] = high
        xlow_ref[pl.ds(plane * slices, slices), :bunch_dev] = low

    moment_copy = pltpu.make_async_copy(moments_ref, moments_hbm, sems.at[5])
    moment_copy.start()
    copies[4].wait()
    def spread(turn, carry):
        at = pl.ds(pl.multiple_of(turn * bunch_dev, bunch_dev), bunch_dev)
        xhigh_ref[:, at], xlow_ref[:, at] = split(history_ref[turn - 1])
        return carry

    for turn in range(1, turns):
        spread(turn, 0)

    parity = odd_ref[0]
    half = trains // 2

    def reach(block, carry):
        at = pl.ds(pl.multiple_of(2 * block * bunch_dev, 2 * bunch_dev), 2 * bunch_dev)
        out = wide_dot((xhigh_ref[...], xlow_ref[...]), (high_ref[:, at], low_ref[:, at]))
        slot = lax.rem(block + parity, half)
        for plane, (keep_ref, send_ref) in enumerate(((keep0_ref, send0_ref), (keep1_ref, send1_ref))):
            part = out[plane * slices : (plane + 1) * slices]
            keep_ref[block] = part[:, :bunch_dev]
            send_ref[slot] = part[:, bunch_dev:]
        return carry

    for block in range(half):
        reach(block, 0)
    moment_copy.wait()


def track_kernel(plane, coef_ref, coord_ref, index_ref, wake_ref, part_refs, kick_ref, store, finish):
    bunch_dev = wake_ref.shape[0]
    chunks = index_ref.shape[0] // bunch_dev
    field = part_refs[0][...]
    for ref in part_refs[1:]:
        field = field + ref[...]
    kick_ref[...] = wide_dot(split(field.T), split(wake_ref[...].T))
    tune, detune = coef_ref[plane], coef_ref[2 + plane]

    def group(step, carry):
        table = kick_ref[pl.ds(pl.multiple_of(step * 8, 8), 8), :]
        for chunk in range(chunks):
            picked = index_ref[pl.ds(step * 8 * chunks + chunk, 8, stride=chunks), :]
            start = step * 32 * chunks + 4 * chunk + 2 * plane
            push = jnp.take_along_axis(table, picked, axis=1)
            position = coord_ref[pl.ds(start, 8, stride=4 * chunks), :]
            slope = coord_ref[pl.ds(start + 1, 8, stride=4 * chunks), :] + push
            square = position * position + slope * slope
            cosine, sine = rotation(tune + detune * square)
            store(step, chunk, cosine * position + sine * slope, cosine * slope - sine * position)
        return carry

    steps = bunch_dev // 8
    for piece in range(4):
        lax.fori_loop(piece * steps // 4, (piece + 1) * steps // 4, group, 0)
        finish(piece)


def first_kernel(coef_ref, coord_ref, index_ref, wake_ref, *rest):
    part_refs, (moved_ref, kick_ref) = rest[:-2], rest[-2:]
    chunks = index_ref.shape[0] // wake_ref.shape[0]

    def store(step, chunk, position, slope):
        at = pl.ds(step * 8 * chunks + chunk, 8, stride=chunks)
        moved_ref[0, at, :] = position
        moved_ref[1, at, :] = slope

    track_kernel(0, coef_ref, coord_ref, index_ref, wake_ref, part_refs, kick_ref, store, lambda piece: None)


def second_kernel(coef_ref, coord_ref, index_ref, wake_ref, first_ref, *rest):
    part_refs, (moved_hbm, kick_ref, moved_ref, sems) = rest[:-4], rest[-4:]
    bunch_dev = wake_ref.shape[0]
    chunks = index_ref.shape[0] // bunch_dev
    copies = []

    def store(step, chunk, position, slope):
        start = step * 32 * chunks + 4 * chunk
        source = pl.ds(step * 8 * chunks + chunk, 8, stride=chunks)
        moved = (first_ref[0, source, :], first_ref[1, source, :], position, slope)
        for i in range(4):
            moved_ref[pl.ds(start + i, 8, stride=4 * chunks), :] = moved[i]

    def finish(piece):
        span = pl.ds(piece * bunch_dev * chunks, bunch_dev * chunks)
        copies.append(pltpu.make_async_copy(moved_ref.at[span], moved_hbm.at[span], sems.at[piece]))
        copies[-1].start()

    track_kernel(1, coef_ref, coord_ref, index_ref, wake_ref, part_refs, kick_ref, store, finish)
    for copy in copies:
        copy.wait()


def staged(coordinates, slice_index, history, impedance, slice_wake, tunes, detuning):
    turn_total, _, slice_count, bunch_dev = history.shape
    trains = lax.axis_size("train")
    bunch_total = trains * bunch_dev
    half = trains // 2
    lanes = 128
    columns = slice_index.shape[0] // lanes
    grid = coordinates.reshape(4, columns, lanes).transpose(1, 0, 2).reshape(4 * columns, lanes)
    picked = slice_index.reshape(columns, lanes)
    stacked = history.reshape(turn_total, 2 * slice_count, bunch_dev)
    rows = impedance.reshape(turn_total + 1, 2, trains, bunch_dev).transpose(0, 2, 1, 3)
    rows = rows.reshape((turn_total + 1) * 2 * trains, bunch_dev)
    fine = wave_table(trains, bunch_dev)
    odd = lax.rem(lax.axis_index("train"), 2).reshape(1)
    vmem = pl.BlockSpec(memory_space=pltpu.VMEM)
    smem = pl.BlockSpec(memory_space=pltpu.SMEM)
    hbm = pl.BlockSpec(memory_space=pltpu.HBM)
    block = jax.ShapeDtypeStruct((half, slice_count, bunch_dev), jnp.float32)
    depth = (turn_total + 1) * bunch_dev
    moments, keep0, keep1, send0, send1 = pl.pallas_call(
        front_kernel,
        out_shape=(jax.ShapeDtypeStruct((2, slice_count, bunch_dev), jnp.float32), block, block, block, block),
        in_specs=[smem] + [hbm] * 5,
        out_specs=[hbm] + [vmem] * 4,
        scratch_shapes=[
            pltpu.VMEM((2, slice_count, bunch_dev), jnp.float32),
            pltpu.VMEM((depth, bunch_total), jnp.bfloat16),
            pltpu.VMEM((depth, bunch_total), jnp.bfloat16),
            pltpu.VMEM((2 * slice_count, depth), jnp.bfloat16),
            pltpu.VMEM((2 * slice_count, depth), jnp.bfloat16),
            pltpu.VMEM(grid.shape, jnp.float32),
            pltpu.VMEM(picked.shape, jnp.int32),
            pltpu.VMEM(stacked.shape, jnp.float32),
            pltpu.VMEM((2, bunch_dev, slice_count), jnp.float32),
            pltpu.VMEM((rows.shape[0], 2 * bunch_total), jnp.float32),
            pltpu.VMEM(rows.shape, jnp.float32),
            pltpu.VMEM(fine.shape, jnp.bfloat16),
            pltpu.SemaphoreType.DMA((6,)),
        ],
        compiler_params=pltpu.CompilerParams(vmem_limit_bytes=40 * 2**20),
        name="front",
    )(odd, *[pltpu.with_memory_space_constraint(x, pltpu.HBM) for x in (grid, picked, stacked, rows, fine)])

    pairs = [(i, i ^ 1) for i in range(trains)]
    parts = []
    for keep, send in ((keep0, send0), (keep1, send1)):
        far = lax.ppermute(send, "train", pairs)
        near = [keep[hop] + far[hop] for hop in range(half)]
        mine = [near[0]]
        for hop in range(1, half):
            shift = [(i, (i + 2 * hop) % trains) for i in range(trains)]
            mine.append(lax.ppermute(near[hop], "train", shift))
        parts.append(mine)
    marked = lax.optimization_barrier((tunes, detuning, parts[0][1]))
    coefs = jnp.concatenate([marked[0] * 4.0, marked[1] * (1.0 / math.pi)])
    parts[0][1] = marked[2]

    estimate = pl.CostEstimate(flops=2 * 10**9, transcendentals=0, bytes_accessed=10**6)
    first = pl.pallas_call(
        first_kernel,
        out_shape=jax.ShapeDtypeStruct((2,) + picked.shape, jnp.float32),
        in_specs=[smem] + [vmem] * (3 + half),
        out_specs=vmem,
        scratch_shapes=[pltpu.VMEM((bunch_dev, slice_count), jnp.float32)],
        compiler_params=pltpu.CompilerParams(vmem_limit_bytes=16 * 2**20),
        cost_estimate=estimate,
        name="first",
    )(coefs, grid, picked, slice_wake, *parts[0])
    moved = pl.pallas_call(
        second_kernel,
        out_shape=jax.ShapeDtypeStruct(grid.shape, jnp.float32),
        in_specs=[smem] + [vmem] * (4 + half),
        out_specs=hbm,
        scratch_shapes=[
            pltpu.VMEM((bunch_dev, slice_count), jnp.float32),
            pltpu.VMEM(grid.shape, jnp.float32),
            pltpu.SemaphoreType.DMA((4,)),
        ],
        compiler_params=pltpu.CompilerParams(vmem_limit_bytes=16 * 2**20),
        cost_estimate=estimate,
        name="second",
    )(coefs, grid, picked, slice_wake, first, *parts[1])
    tracked = moved.reshape(columns, 4, lanes).transpose(1, 0, 2).reshape(4, columns * lanes)
    return (tracked, moments)


def local(coordinates, slice_index, history, impedance, slice_wake, tunes, detuning):
    trains = lax.axis_size("train")
    slice_count, bunch_dev = history.shape[2:]
    per_bunch = slice_index.shape[0] // bunch_dev
    fits = slice_count == bunch_dev == 128 and per_bunch % 128 == 0 and trains % 2 == 0 and trains <= 16
    body = staged if fits else generic
    return body(coordinates, slice_index, history, impedance, slice_wake, tunes, detuning)


def solution(mesh):
    return jax.shard_map(
        local,
        mesh=mesh,
        in_specs=(
            P("seed", "train"),
            P(("seed", "train")),
            P("seed", None, None, "train"),
            P(),
            P(),
            P("seed"),
            P("seed"),
        ),
        out_specs=(P("seed", "train"), P("seed", None, "train")),
        check_vma=False,
    )
```

```python
import math

import jax
import jax.numpy as jnp
import numpy as np
from jax import lax
from jax.experimental import pallas as pl
from jax.experimental.pallas import tpu as pltpu
from jax.sharding import PartitionSpec as P


full_turn = 2.0 * math.pi


def rotate(positions, pushes, tunes, detuning):
    result = []
    for plane_index in range(2):
        position = positions[2 * plane_index]
        slope = positions[2 * plane_index + 1] + pushes[plane_index]
        action = 0.5 * (position * position + slope * slope)
        phase = full_turn * tunes[plane_index] + detuning[plane_index] * action
        cosine = jnp.cos(phase)
        sine = jnp.sin(phase)
        result.append(cosine * position + sine * slope)
        result.append(cosine * slope - sine * position)
    return jnp.stack(result)


def phase_tables(row_count, col_count, period):
    first = lax.broadcasted_iota(jnp.int32, (row_count, col_count), 0)
    second = lax.broadcasted_iota(jnp.int32, (row_count, col_count), 1)
    angle = full_turn / period * (first * second % period).astype(jnp.float32)
    return (jnp.cos(angle), jnp.sin(angle))


def contract(form, table, values):
    return jnp.einsum(form, table, values, precision=lax.Precision.HIGHEST)


def forward(series):
    item_count, column_count, bunch_total = series.shape
    trains = lax.axis_size("train")
    bunch_dev = bunch_total // trains
    signal = series.reshape(item_count, column_count, trains, bunch_dev)
    cos_train, sin_train = phase_tables(trains, trains, trains)
    first_re = contract("kp,ncpj->nckj", cos_train, signal)
    first_im = -contract("kp,ncpj->nckj", sin_train, signal)
    cos_twist, sin_twist = phase_tables(trains, bunch_dev, bunch_total)
    twist_re = first_re * cos_twist + first_im * sin_twist
    twist_im = first_im * cos_twist - first_re * sin_twist
    cos_local, sin_local = phase_tables(bunch_dev, bunch_dev, bunch_dev)
    spec_re = contract("qj,nckj->ncqk", cos_local, twist_re) + contract(
        "qj,nckj->ncqk", sin_local, twist_im
    )
    spec_im = contract("qj,nckj->ncqk", cos_local, twist_im) - contract(
        "qj,nckj->ncqk", sin_local, twist_re
    )
    return (
        spec_re.reshape(item_count, column_count, bunch_total),
        spec_im.reshape(item_count, column_count, bunch_total),
    )


def inverse(summed_re, summed_im):
    column_count, bunch_total = summed_re.shape
    trains = lax.axis_size("train")
    bunch_dev = bunch_total // trains
    grid_re = summed_re.reshape(column_count, bunch_dev, trains)
    grid_im = summed_im.reshape(column_count, bunch_dev, trains)
    cos_local, sin_local = phase_tables(bunch_dev, bunch_dev, bunch_dev)
    back_re = contract("qj,cqk->ckj", cos_local, grid_re) - contract(
        "qj,cqk->ckj", sin_local, grid_im
    )
    back_im = contract("qj,cqk->ckj", cos_local, grid_im) + contract(
        "qj,cqk->ckj", sin_local, grid_re
    )
    cos_twist, sin_twist = phase_tables(trains, bunch_dev, bunch_total)
    turned_re = back_re * cos_twist - back_im * sin_twist
    turned_im = back_re * sin_twist + back_im * cos_twist
    cos_train, sin_train = phase_tables(trains, trains, trains)
    field = (
        contract("kp,ckj->cpj", cos_train, turned_re)
        - contract("kp,ckj->cpj", sin_train, turned_im)
    ) / bunch_total
    return field.reshape(column_count, bunch_total)


def generic(coordinates, slice_index, history, impedance, slice_wake, tunes, detuning):
    particle_count = slice_index.shape[0]
    slice_count = slice_wake.shape[0]
    bunch_dev = history.shape[3]
    turn_total = history.shape[0] + 1
    per_bunch = particle_count // bunch_dev
    bunch_group = math.gcd(bunch_dev, 16)
    group_count = bunch_dev // bunch_group
    group_span = bunch_group * per_bunch
    levels = lax.broadcasted_iota(jnp.int32, (1, 1, slice_count), 2)

    def selector(group_index):
        picked = lax.dynamic_slice_in_dim(slice_index, group_index * group_span, group_span)
        picked = picked.reshape(bunch_group, per_bunch)
        return (picked[:, :, None] == levels).astype(jnp.float32)

    def deposit(group_index, gathered):
        onehot = selector(group_index)
        section = lax.dynamic_slice_in_dim(coordinates, group_index * group_span, group_span, 1)
        transverse = section[0::2].reshape(2, bunch_group, per_bunch)
        sums = contract("gps,cgp->csg", onehot, transverse)
        return lax.dynamic_update_slice_in_dim(
            gathered, sums * (slice_count / per_bunch), group_index * bunch_group, 2
        )

    moments = lax.fori_loop(
        0, group_count, deposit, jnp.zeros((2, slice_count, bunch_dev), jnp.float32)
    )
    series = jnp.concatenate([moments[None], history], 0).reshape(
        turn_total, 2 * slice_count, bunch_dev
    )
    imp_re = impedance[:, 0, :]
    imp_im = impedance[:, 1, :]
    spec_re, spec_im = forward(
        lax.all_to_all(series, "train", split_axis=1, concat_axis=2, tiled=True)
    )
    summed_re = jnp.sum(imp_re[:, None, :] * spec_re - imp_im[:, None, :] * spec_im, axis=0)
    summed_im = jnp.sum(imp_re[:, None, :] * spec_im + imp_im[:, None, :] * spec_re, axis=0)
    field = inverse(summed_re, summed_im)
    home = lax.all_to_all(field, "train", split_axis=1, concat_axis=0, tiled=True).reshape(
        2, slice_count, bunch_dev
    )
    kicks = contract("st,ctb->csb", slice_wake, home)

    def track(group_index, moved):
        onehot = selector(group_index)
        local_kicks = lax.dynamic_slice_in_dim(kicks, group_index * bunch_group, bunch_group, 2)
        pushes = contract("gps,csg->cgp", onehot, local_kicks).reshape(2, group_span)
        section = lax.dynamic_slice_in_dim(coordinates, group_index * group_span, group_span, 1)
        turned = rotate(section, pushes, tunes, detuning)
        return lax.dynamic_update_slice_in_dim(moved, turned, group_index * group_span, 1)

    tracked = lax.fori_loop(0, group_count, track, jnp.zeros_like(coordinates))
    return (tracked, moments)


def split(values):
    high = values.astype(jnp.bfloat16)
    return high, (values - high.astype(jnp.float32)).astype(jnp.bfloat16)


def wide_dot(left, right):
    total = jnp.dot(left[0], right[0], preferred_element_type=jnp.float32)
    total += jnp.dot(left[0], right[1], preferred_element_type=jnp.float32)
    return total + jnp.dot(left[1], right[0], preferred_element_type=jnp.float32)


def wave_table(trains, bunch_dev):
    total = trains * bunch_dev
    q = np.arange(bunch_dev)[:, None]
    n = np.arange(total)[None, :]
    angle = full_turn / total * (q * n % total)
    fine = np.float32(np.concatenate([np.cos(angle), np.sin(angle)], 1))
    fine_high = fine.astype(jnp.bfloat16)
    fine_low = (fine - fine_high.astype(np.float32)).astype(jnp.bfloat16)
    return np.stack([fine_high, fine_low])


def rotation(turn_quarters):
    whole = jnp.round(turn_quarters)
    rest = turn_quarters - whole
    square = rest * rest
    sine = rest * (1.5707963267948966 + square * (-0.6459640975062462 + square * (
        0.07969262624616703 + square * (-0.004681754135318687 + square * 0.00016044118478735982))))
    cosine = 1.0 + square * (-1.2337005501361697 + square * (0.253669507901048 + square * (
        -0.02086348076335296 + square * (0.0009192602748394264 + square * -0.000025202042373060603))))
    quadrant = whole.astype(jnp.int32)
    swap = (quadrant & 1) == 1
    cos_abs = jnp.where(swap, sine, cosine)
    sin_abs = jnp.where(swap, cosine, sine)
    cos_out = jnp.where(((quadrant + 1) & 2) == 2, -cos_abs, cos_abs)
    sin_out = jnp.where((quadrant & 2) == 2, -sin_abs, sin_abs)
    return cos_out, sin_out


def swap_bits(blocks, lane):
    for step in (1, 2, 4):
        low = (lane & step) == 0
        for i in range(8):
            if not i & step:
                first, second = blocks[i], blocks[i | step]
                blocks[i] = jnp.where(low, first, pltpu.roll(second, step, 1))
                blocks[i | step] = jnp.where(low, pltpu.roll(first, 128 - step, 1), second)
    return blocks


def front_kernel(
    place_ref, coord_hbm, index_hbm, history_hbm, impedance_hbm, fine_hbm,
    moments_hbm, keep0_ref, keep1_ref, send0_ref, send1_ref,
    moments_ref, high_ref, low_ref, xhigh_ref, xlow_ref, coord_ref, index_ref, history_ref, group_ref, waves_ref, impedance_ref, fine_ref, sems,
):
    turns = history_ref.shape[0] + 1
    bunch_dev = history_ref.shape[2]
    total = high_ref.shape[1]
    trains = total // bunch_dev
    slices = moments_ref.shape[1]
    chunks = index_ref.shape[0] // bunch_dev
    copies = [
        pltpu.make_async_copy(source, target, sems.at[i])
        for i, (source, target) in enumerate(
            ((impedance_hbm, impedance_ref), (fine_hbm, fine_ref), (index_hbm, index_ref), (coord_hbm, coord_ref),
             (history_hbm, history_ref))
        )
    ]
    for copy in copies:
        copy.start()

    copies[0].wait()
    copies[1].wait()
    high, low = split(impedance_ref[...])

    def wave(block, carry):
        at = pl.ds(pl.multiple_of(block * 256, 256), 256)
        waves_ref[:, at] = wide_dot((high, low), (fine_ref[0, :, at], fine_ref[1, :, at]))
        return carry

    for block in range(2 * total // 256):
        wave(block, 0)
    row = lax.broadcasted_iota(jnp.int32, (8, bunch_dev), 0)
    lane = lax.broadcasted_iota(jnp.int32, (8, bunch_dev), 1)
    r = lax.broadcasted_iota(jnp.int32, (2 * trains, bunch_dev), 0)
    n = lax.broadcasted_iota(jnp.int32, (2 * trains, bunch_dev), 1)
    cosine, sine = rotation(lax.rem((r >> 1) * n, trains).astype(jnp.float32) * (4.0 / trains))
    real = (r & 1) == 0
    coarse_cos = jnp.where(real, cosine, -sine) * (1.0 / total)
    coarse_sin = jnp.where(real, -sine, -cosine) * (1.0 / total)
    def circulant(turn, carry):
        rows = pl.ds(pl.multiple_of(turn * 2 * trains, 2 * trains), 2 * trains)
        pieces = []
        for block in range(trains):
            on_cos = waves_ref[rows, pl.ds(block * bunch_dev, bunch_dev)] * coarse_cos
            on_sin = waves_ref[rows, pl.ds(total + block * bunch_dev, bunch_dev)] * coarse_sin
            piece = jnp.sum(on_cos + on_sin, 0, keepdims=True)
            pieces.append(jnp.broadcast_to(piece, (8, bunch_dev)))
        for m in range(bunch_dev // 16):
            parts = []
            for shift in (16 * m, 16 * m + 8):
                inside = lane >= row + shift
                turned = [pltpu.roll(piece, shift, 1, stride=1, stride_axis=0) for piece in pieces]
                parts.append([jnp.where(inside, turned[d], turned[d - 1]) for d in range(trains)])
            at = pl.multiple_of(turn * bunch_dev + 16 * m, 16)
            for d in range(trains):
                high, low = split(jnp.concatenate([parts[0][d], parts[1][d]], 0))
                high_ref[pl.ds(at, 16), pl.ds(d * bunch_dev, bunch_dev)] = high
                low_ref[pl.ds(at, 16), pl.ds(d * bunch_dev, bunch_dev)] = low
        return carry

    for turn in range(turns):
        circulant(turn, 0)
    copies[2].wait()
    copies[3].wait()
    digit = lax.broadcasted_iota(jnp.int32, (16, 128), 0)
    octal = lax.broadcasted_iota(jnp.int32, (8, 128), 0)

    owner = lax.broadcasted_iota(jnp.int32, (16, 128), 1) >> 4

    def deposit(group, carry):
        lows, values = [], []
        for inner in range(8):
            bunch = group * 8 + inner
            low_rows, value_rows = [], []
            for chunk in range(chunks):
                place = index_ref[pl.ds(bunch * chunks + chunk, 1), :]
                low_rows.append(jnp.where(digit == (place & 15), 1.0, 0.0))
                hit = octal == (place >> 4)
                base = (bunch * chunks + chunk) * 4
                value_rows.append(jnp.concatenate([
                    jnp.where(hit, coord_ref[pl.ds(base + 2 * plane, 1), :], 0.0) for plane in range(2)
                ], 0))
            lows.append(jnp.concatenate(low_rows, 1).astype(jnp.bfloat16))
            values.append(jnp.concatenate(value_rows, 1))
        both = jnp.concatenate(split(jnp.concatenate(values, 0)), 0)
        out = lax.dot_general(
            both, jnp.concatenate(lows, 0), (((1,), (1,)), ((), ())), preferred_element_type=jnp.float32
        )
        placed = jnp.zeros((16, 128), jnp.float32)
        for inner in range(8):
            at = 16 * inner
            placed = jnp.where(owner == inner, out[at : at + 16] + out[128 + at : 144 + at], placed)
        at = pl.ds(pl.multiple_of(group * 8, 8), 8)
        group_ref[0, at, :] = placed[:8]
        group_ref[1, at, :] = placed[8:]
        return carry

    lax.fori_loop(0, bunch_dev // 8, deposit, 0, unroll=16)
    lanes16 = lax.broadcasted_iota(jnp.int32, (16, 128), 1)
    for plane in range(2):
        turned = group_ref[plane].T
        blocks = swap_bits([turned[16 * i : 16 * i + 16] for i in range(8)], lanes16)
        current = jnp.concatenate(blocks, 0) * (slices / (chunks * 128))
        moments_ref[plane] = current
        high, low = split(current)
        xhigh_ref[pl.ds(plane * slices, slices), :bunch_dev] = high
        xlow_ref[pl.ds(plane * slices, slices), :bunch_dev] = low

    moment_copy = pltpu.make_async_copy(moments_ref, moments_hbm, sems.at[5])
    moment_copy.start()
    copies[4].wait()
    def spread(turn, carry):
        at = pl.ds(pl.multiple_of(turn * bunch_dev, bunch_dev), bunch_dev)
        xhigh_ref[:, at], xlow_ref[:, at] = split(history_ref[turn - 1])
        return carry

    for turn in range(1, turns):
        spread(turn, 0)

    place = place_ref[0]
    half = trains // 2

    def reach(block, carry):
        at = pl.ds(pl.multiple_of(2 * block * bunch_dev, 2 * bunch_dev), 2 * bunch_dev)
        out = wide_dot((xhigh_ref[...], xlow_ref[...]), (high_ref[:, at], low_ref[:, at]))
        keep_slot, send_slot = [(place >> 1) ^ (lax.rem(place + 2 * block + odd, trains) >> 1) for odd in range(2)]
        for plane, (keep_ref, send_ref) in enumerate(((keep0_ref, send0_ref), (keep1_ref, send1_ref))):
            part = out[plane * slices : (plane + 1) * slices]
            keep_ref[keep_slot] = part[:, :bunch_dev]
            send_ref[send_slot] = part[:, bunch_dev:]
        return carry

    for block in range(half):
        reach(block, 0)
    moment_copy.wait()


def track_kernel(plane, coef_ref, coord_ref, index_ref, wake_ref, part_refs, kick_ref, store, finish):
    bunch_dev = wake_ref.shape[0]
    chunks = index_ref.shape[0] // bunch_dev
    field = part_refs[0][...]
    for ref in part_refs[1:]:
        field = field + ref[...]
    kick_ref[...] = wide_dot(split(field.T), split(wake_ref[...].T))
    tune, detune = coef_ref[plane], coef_ref[2 + plane]

    def group(step, carry):
        table = kick_ref[pl.ds(pl.multiple_of(step * 8, 8), 8), :]
        for chunk in range(chunks):
            picked = index_ref[pl.ds(step * 8 * chunks + chunk, 8, stride=chunks), :]
            start = step * 32 * chunks + 4 * chunk + 2 * plane
            push = jnp.take_along_axis(table, picked, axis=1)
            position = coord_ref[pl.ds(start, 8, stride=4 * chunks), :]
            slope = coord_ref[pl.ds(start + 1, 8, stride=4 * chunks), :] + push
            square = position * position + slope * slope
            cosine, sine = rotation(tune + detune * square)
            store(step, chunk, cosine * position + sine * slope, cosine * slope - sine * position)
        return carry

    steps = bunch_dev // 8
    for piece in range(4):
        lax.fori_loop(piece * steps // 4, (piece + 1) * steps // 4, group, 0, unroll=4)
        finish(piece)


def first_kernel(coef_ref, coord_ref, index_ref, wake_ref, *rest):
    part_refs, (moved_ref, kick_ref) = rest[:-2], rest[-2:]
    chunks = index_ref.shape[0] // wake_ref.shape[0]

    def store(step, chunk, position, slope):
        at = pl.ds(step * 8 * chunks + chunk, 8, stride=chunks)
        moved_ref[0, at, :] = position
        moved_ref[1, at, :] = slope

    track_kernel(0, coef_ref, coord_ref, index_ref, wake_ref, part_refs, kick_ref, store, lambda piece: None)


def second_kernel(coef_ref, coord_ref, index_ref, wake_ref, first_ref, *rest):
    part_refs, (moved_hbm, kick_ref, moved_ref, sems) = rest[:-4], rest[-4:]
    bunch_dev = wake_ref.shape[0]
    chunks = index_ref.shape[0] // bunch_dev
    copies = []

    def store(step, chunk, position, slope):
        start = step * 32 * chunks + 4 * chunk
        source = pl.ds(step * 8 * chunks + chunk, 8, stride=chunks)
        moved = (first_ref[0, source, :], first_ref[1, source, :], position, slope)
        for i in range(4):
            moved_ref[pl.ds(start + i, 8, stride=4 * chunks), :] = moved[i]

    def finish(piece):
        span = pl.ds(piece * bunch_dev * chunks, bunch_dev * chunks)
        copies.append(pltpu.make_async_copy(moved_ref.at[span], moved_hbm.at[span], sems.at[piece]))
        copies[-1].start()

    track_kernel(1, coef_ref, coord_ref, index_ref, wake_ref, part_refs, kick_ref, store, finish)
    for copy in copies:
        copy.wait()


def staged(coordinates, slice_index, history, impedance, slice_wake, tunes, detuning):
    turn_total, _, slice_count, bunch_dev = history.shape
    trains = lax.axis_size("train")
    bunch_total = trains * bunch_dev
    half = trains // 2
    lanes = 128
    columns = slice_index.shape[0] // lanes
    grid = coordinates.reshape(4, columns, lanes).transpose(1, 0, 2).reshape(4 * columns, lanes)
    picked = slice_index.reshape(columns, lanes)
    stacked = history.reshape(turn_total, 2 * slice_count, bunch_dev)
    rows = impedance.reshape(turn_total + 1, 2, trains, bunch_dev).transpose(0, 2, 1, 3)
    rows = rows.reshape((turn_total + 1) * 2 * trains, bunch_dev)
    fine = wave_table(trains, bunch_dev)
    place = lax.axis_index("train").reshape(1)
    vmem = pl.BlockSpec(memory_space=pltpu.VMEM)
    smem = pl.BlockSpec(memory_space=pltpu.SMEM)
    hbm = pl.BlockSpec(memory_space=pltpu.HBM)
    block = jax.ShapeDtypeStruct((half, slice_count, bunch_dev), jnp.float32)
    depth = (turn_total + 1) * bunch_dev
    moments, keep0, keep1, send0, send1 = pl.pallas_call(
        front_kernel,
        out_shape=(jax.ShapeDtypeStruct((2, slice_count, bunch_dev), jnp.float32), block, block, block, block),
        in_specs=[smem] + [hbm] * 5,
        out_specs=[hbm] + [vmem] * 4,
        scratch_shapes=[
            pltpu.VMEM((2, slice_count, bunch_dev), jnp.float32),
            pltpu.VMEM((depth, bunch_total), jnp.bfloat16),
            pltpu.VMEM((depth, bunch_total), jnp.bfloat16),
            pltpu.VMEM((2 * slice_count, depth), jnp.bfloat16),
            pltpu.VMEM((2 * slice_count, depth), jnp.bfloat16),
            pltpu.VMEM(grid.shape, jnp.float32),
            pltpu.VMEM(picked.shape, jnp.int32),
            pltpu.VMEM(stacked.shape, jnp.float32),
            pltpu.VMEM((2, bunch_dev, slice_count), jnp.float32),
            pltpu.VMEM((rows.shape[0], 2 * bunch_total), jnp.float32),
            pltpu.VMEM(rows.shape, jnp.float32),
            pltpu.VMEM(fine.shape, jnp.bfloat16),
            pltpu.SemaphoreType.DMA((6,)),
        ],
        compiler_params=pltpu.CompilerParams(vmem_limit_bytes=40 * 2**20),
        name="front",
    )(place, *[pltpu.with_memory_space_constraint(x, pltpu.HBM) for x in (grid, picked, stacked, rows, fine)])

    pairs = [(i, i ^ 1) for i in range(trains)]
    parts = []
    for keep, send in ((keep0, send0), (keep1, send1)):
        far = lax.ppermute(send, "train", pairs)
        near = [keep[hop] + far[hop] for hop in range(half)]
        mine = [near[0]]
        for hop in [*range(max(1, half // 2), half), *range(1, half // 2)][::-1]:
            shift = [(i, i ^ (2 * hop)) for i in range(trains)]
            mine.append(lax.ppermute(near[hop], "train", shift))
        parts.append(mine)
    marked = lax.optimization_barrier((tunes, detuning, parts[0][1]))
    coefs = jnp.concatenate([marked[0] * 4.0, marked[1] * (1.0 / math.pi)])
    parts[0][1] = marked[2]

    estimate = pl.CostEstimate(flops=2 * 10**9, transcendentals=0, bytes_accessed=10**6)
    first = pl.pallas_call(
        first_kernel,
        out_shape=jax.ShapeDtypeStruct((2,) + picked.shape, jnp.float32),
        in_specs=[smem] + [vmem] * (3 + half),
        out_specs=vmem,
        scratch_shapes=[pltpu.VMEM((bunch_dev, slice_count), jnp.float32)],
        compiler_params=pltpu.CompilerParams(vmem_limit_bytes=16 * 2**20),
        cost_estimate=estimate,
        name="first",
    )(coefs, grid, picked, slice_wake, *parts[0])
    moved = pl.pallas_call(
        second_kernel,
        out_shape=jax.ShapeDtypeStruct(grid.shape, jnp.float32),
        in_specs=[smem] + [vmem] * (4 + half),
        out_specs=hbm,
        scratch_shapes=[
            pltpu.VMEM((bunch_dev, slice_count), jnp.float32),
            pltpu.VMEM(grid.shape, jnp.float32),
            pltpu.SemaphoreType.DMA((4,)),
        ],
        compiler_params=pltpu.CompilerParams(vmem_limit_bytes=16 * 2**20),
        cost_estimate=estimate,
        name="second",
    )(coefs, grid, picked, slice_wake, first, *parts[1])
    tracked = moved.reshape(columns, 4, lanes).transpose(1, 0, 2).reshape(4, columns * lanes)
    return (tracked, moments)


def local(coordinates, slice_index, history, impedance, slice_wake, tunes, detuning):
    trains = lax.axis_size("train")
    slice_count, bunch_dev = history.shape[2:]
    per_bunch = slice_index.shape[0] // bunch_dev
    fits = slice_count == bunch_dev == 128 and per_bunch % 128 == 0 and trains in (2, 4, 8, 16)
    body = staged if fits else generic
    return body(coordinates, slice_index, history, impedance, slice_wake, tunes, detuning)


def solution(mesh):
    return jax.shard_map(
        local,
        mesh=mesh,
        in_specs=(
            P("seed", "train"),
            P(("seed", "train")),
            P("seed", None, None, "train"),
            P(),
            P(),
            P("seed"),
            P("seed"),
        ),
        out_specs=(P("seed", "train"), P("seed", None, "train")),
        check_vma=False,
    )
```

```python
import math

import jax
import jax.numpy as jnp
import numpy as np
from jax import lax
from jax.experimental import pallas as pl
from jax.experimental.pallas import tpu as pltpu
from jax.sharding import PartitionSpec as P


full_turn = 2.0 * math.pi


def rotate(positions, pushes, tunes, detuning):
    result = []
    for plane_index in range(2):
        position = positions[2 * plane_index]
        slope = positions[2 * plane_index + 1] + pushes[plane_index]
        action = 0.5 * (position * position + slope * slope)
        phase = full_turn * tunes[plane_index] + detuning[plane_index] * action
        cosine = jnp.cos(phase)
        sine = jnp.sin(phase)
        result.append(cosine * position + sine * slope)
        result.append(cosine * slope - sine * position)
    return jnp.stack(result)


def phase_tables(row_count, col_count, period):
    first = lax.broadcasted_iota(jnp.int32, (row_count, col_count), 0)
    second = lax.broadcasted_iota(jnp.int32, (row_count, col_count), 1)
    angle = full_turn / period * (first * second % period).astype(jnp.float32)
    return (jnp.cos(angle), jnp.sin(angle))


def contract(form, table, values):
    return jnp.einsum(form, table, values, precision=lax.Precision.HIGHEST)


def forward(series):
    item_count, column_count, bunch_total = series.shape
    trains = lax.axis_size("train")
    bunch_dev = bunch_total // trains
    signal = series.reshape(item_count, column_count, trains, bunch_dev)
    cos_train, sin_train = phase_tables(trains, trains, trains)
    first_re = contract("kp,ncpj->nckj", cos_train, signal)
    first_im = -contract("kp,ncpj->nckj", sin_train, signal)
    cos_twist, sin_twist = phase_tables(trains, bunch_dev, bunch_total)
    twist_re = first_re * cos_twist + first_im * sin_twist
    twist_im = first_im * cos_twist - first_re * sin_twist
    cos_local, sin_local = phase_tables(bunch_dev, bunch_dev, bunch_dev)
    spec_re = contract("qj,nckj->ncqk", cos_local, twist_re) + contract(
        "qj,nckj->ncqk", sin_local, twist_im
    )
    spec_im = contract("qj,nckj->ncqk", cos_local, twist_im) - contract(
        "qj,nckj->ncqk", sin_local, twist_re
    )
    return (
        spec_re.reshape(item_count, column_count, bunch_total),
        spec_im.reshape(item_count, column_count, bunch_total),
    )


def inverse(summed_re, summed_im):
    column_count, bunch_total = summed_re.shape
    trains = lax.axis_size("train")
    bunch_dev = bunch_total // trains
    grid_re = summed_re.reshape(column_count, bunch_dev, trains)
    grid_im = summed_im.reshape(column_count, bunch_dev, trains)
    cos_local, sin_local = phase_tables(bunch_dev, bunch_dev, bunch_dev)
    back_re = contract("qj,cqk->ckj", cos_local, grid_re) - contract(
        "qj,cqk->ckj", sin_local, grid_im
    )
    back_im = contract("qj,cqk->ckj", cos_local, grid_im) + contract(
        "qj,cqk->ckj", sin_local, grid_re
    )
    cos_twist, sin_twist = phase_tables(trains, bunch_dev, bunch_total)
    turned_re = back_re * cos_twist - back_im * sin_twist
    turned_im = back_re * sin_twist + back_im * cos_twist
    cos_train, sin_train = phase_tables(trains, trains, trains)
    field = (
        contract("kp,ckj->cpj", cos_train, turned_re)
        - contract("kp,ckj->cpj", sin_train, turned_im)
    ) / bunch_total
    return field.reshape(column_count, bunch_total)


def generic(coordinates, slice_index, history, impedance, slice_wake, tunes, detuning):
    particle_count = slice_index.shape[0]
    slice_count = slice_wake.shape[0]
    bunch_dev = history.shape[3]
    turn_total = history.shape[0] + 1
    per_bunch = particle_count // bunch_dev
    bunch_group = math.gcd(bunch_dev, 16)
    group_count = bunch_dev // bunch_group
    group_span = bunch_group * per_bunch
    levels = lax.broadcasted_iota(jnp.int32, (1, 1, slice_count), 2)

    def selector(group_index):
        picked = lax.dynamic_slice_in_dim(slice_index, group_index * group_span, group_span)
        picked = picked.reshape(bunch_group, per_bunch)
        return (picked[:, :, None] == levels).astype(jnp.float32)

    def deposit(group_index, gathered):
        onehot = selector(group_index)
        section = lax.dynamic_slice_in_dim(coordinates, group_index * group_span, group_span, 1)
        transverse = section[0::2].reshape(2, bunch_group, per_bunch)
        sums = contract("gps,cgp->csg", onehot, transverse)
        return lax.dynamic_update_slice_in_dim(
            gathered, sums * (slice_count / per_bunch), group_index * bunch_group, 2
        )

    moments = lax.fori_loop(
        0, group_count, deposit, jnp.zeros((2, slice_count, bunch_dev), jnp.float32)
    )
    series = jnp.concatenate([moments[None], history], 0).reshape(
        turn_total, 2 * slice_count, bunch_dev
    )
    imp_re = impedance[:, 0, :]
    imp_im = impedance[:, 1, :]
    spec_re, spec_im = forward(
        lax.all_to_all(series, "train", split_axis=1, concat_axis=2, tiled=True)
    )
    summed_re = jnp.sum(imp_re[:, None, :] * spec_re - imp_im[:, None, :] * spec_im, axis=0)
    summed_im = jnp.sum(imp_re[:, None, :] * spec_im + imp_im[:, None, :] * spec_re, axis=0)
    field = inverse(summed_re, summed_im)
    home = lax.all_to_all(field, "train", split_axis=1, concat_axis=0, tiled=True).reshape(
        2, slice_count, bunch_dev
    )
    kicks = contract("st,ctb->csb", slice_wake, home)

    def track(group_index, moved):
        onehot = selector(group_index)
        local_kicks = lax.dynamic_slice_in_dim(kicks, group_index * bunch_group, bunch_group, 2)
        pushes = contract("gps,csg->cgp", onehot, local_kicks).reshape(2, group_span)
        section = lax.dynamic_slice_in_dim(coordinates, group_index * group_span, group_span, 1)
        turned = rotate(section, pushes, tunes, detuning)
        return lax.dynamic_update_slice_in_dim(moved, turned, group_index * group_span, 1)

    tracked = lax.fori_loop(0, group_count, track, jnp.zeros_like(coordinates))
    return (tracked, moments)


def split(values):
    high = values.astype(jnp.bfloat16)
    return high, (values - high.astype(jnp.float32)).astype(jnp.bfloat16)


def wide_dot(left, right):
    total = jnp.dot(left[0], right[0], preferred_element_type=jnp.float32)
    total += jnp.dot(left[0], right[1], preferred_element_type=jnp.float32)
    return total + jnp.dot(left[1], right[0], preferred_element_type=jnp.float32)


def wave_table(trains, bunch_dev):
    total = trains * bunch_dev
    q = np.arange(bunch_dev)[:, None]
    n = np.arange(total)[None, :]
    angle = full_turn / total * (q * n % total)
    fine = np.float32(np.concatenate([np.cos(angle), np.sin(angle)], 1))
    fine_high = fine.astype(jnp.bfloat16)
    fine_low = (fine - fine_high.astype(np.float32)).astype(jnp.bfloat16)
    return np.stack([fine_high, fine_low])


def rotation(turn_quarters):
    whole = jnp.round(turn_quarters)
    rest = turn_quarters - whole
    square = rest * rest
    sine = rest * (1.5707963267948966 + square * (-0.6459640975062462 + square * (
        0.07969262624616703 + square * (-0.004681754135318687 + square * 0.00016044118478735982))))
    cosine = 1.0 + square * (-1.2337005501361697 + square * (0.253669507901048 + square * (
        -0.02086348076335296 + square * (0.0009192602748394264 + square * -0.000025202042373060603))))
    quadrant = whole.astype(jnp.int32)
    swap = (quadrant & 1) == 1
    cos_abs = jnp.where(swap, sine, cosine)
    sin_abs = jnp.where(swap, cosine, sine)
    cos_out = jnp.where(((quadrant + 1) & 2) == 2, -cos_abs, cos_abs)
    sin_out = jnp.where((quadrant & 2) == 2, -sin_abs, sin_abs)
    return cos_out, sin_out


def swap_bits(blocks, lane):
    for step in (1, 2, 4):
        low = (lane & step) == 0
        for i in range(8):
            if not i & step:
                first, second = blocks[i], blocks[i | step]
                blocks[i] = jnp.where(low, first, pltpu.roll(second, step, 1))
                blocks[i | step] = jnp.where(low, pltpu.roll(first, 128 - step, 1), second)
    return blocks


def reach(place, left, right, keep_ref, send_ref):
    half, _, bunch_dev = keep_ref.shape
    for block in range(half):
        at = pl.ds(2 * block * bunch_dev, 2 * bunch_dev)
        out = wide_dot([ref[...] for ref in left], [ref[:, at] for ref in right])
        slots = [(place >> 1) ^ (lax.rem(place + 2 * block + odd, 2 * half) >> 1) for odd in range(2)]
        keep_ref[slots[0]] = out[:, :bunch_dev]
        send_ref[slots[1]] = out[:, bunch_dev:]


def back_kernel(place_ref, high_ref, low_ref, later_high_ref, later_low_ref, keep_ref, send_ref):
    reach(place_ref[0], (later_high_ref, later_low_ref), (high_ref, low_ref), keep_ref, send_ref)


def front_kernel(
    place_ref, coord_hbm, index_hbm, history_hbm, impedance_hbm, fine_hbm,
    moments_hbm, keep_ref, send_ref, high_ref, low_ref, later_high_ref, later_low_ref,
    moments_ref, now_high_ref, now_low_ref, coord_ref, index_ref, history_ref, group_ref, waves_ref, impedance_ref, fine_ref, sems,
):
    turns = history_ref.shape[0] + 1
    bunch_dev = history_ref.shape[2]
    total = high_ref.shape[1]
    trains = total // bunch_dev
    slices = moments_ref.shape[1]
    chunks = index_ref.shape[0] // bunch_dev
    copies = [
        pltpu.make_async_copy(source, target, sems.at[i])
        for i, (source, target) in enumerate(
            ((impedance_hbm, impedance_ref), (fine_hbm, fine_ref), (index_hbm, index_ref), (coord_hbm, coord_ref),
             (history_hbm, history_ref))
        )
    ]
    for copy in copies:
        copy.start()

    copies[0].wait()
    copies[1].wait()
    high, low = split(impedance_ref[...])

    def wave(block, carry):
        at = pl.ds(pl.multiple_of(block * 256, 256), 256)
        waves_ref[:, at] = wide_dot((high, low), (fine_ref[0, :, at], fine_ref[1, :, at]))
        return carry

    for block in range(2 * total // 256):
        wave(block, 0)
    row = lax.broadcasted_iota(jnp.int32, (8, bunch_dev), 0)
    lane = lax.broadcasted_iota(jnp.int32, (8, bunch_dev), 1)
    r = lax.broadcasted_iota(jnp.int32, (2 * trains, bunch_dev), 0)
    n = lax.broadcasted_iota(jnp.int32, (2 * trains, bunch_dev), 1)
    cosine, sine = rotation(lax.rem((r >> 1) * n, trains).astype(jnp.float32) * (4.0 / trains))
    real = (r & 1) == 0
    coarse_cos = jnp.where(real, cosine, -sine) * (1.0 / total)
    coarse_sin = jnp.where(real, -sine, -cosine) * (1.0 / total)

    def circulant(turn, carry):
        rows = pl.ds(pl.multiple_of(turn * 2 * trains, 2 * trains), 2 * trains)
        pieces = []
        for block in range(trains):
            on_cos = waves_ref[rows, pl.ds(block * bunch_dev, bunch_dev)] * coarse_cos
            on_sin = waves_ref[rows, pl.ds(total + block * bunch_dev, bunch_dev)] * coarse_sin
            piece = jnp.sum(on_cos + on_sin, 0, keepdims=True)
            pieces.append(jnp.broadcast_to(piece, (8, bunch_dev)))
        for m in range(bunch_dev // 16):
            parts = []
            for shift in (16 * m, 16 * m + 8):
                inside = lane >= row + shift
                turned = [pltpu.roll(piece, shift, 1, stride=1, stride_axis=0) for piece in pieces]
                parts.append([jnp.where(inside, turned[d], turned[d - 1]) for d in range(trains)])
            at = pl.multiple_of(turn * bunch_dev + 16 * m, 16)
            for d in range(trains):
                high, low = split(jnp.concatenate([parts[0][d], parts[1][d]], 0))
                high_ref[pl.ds(at, 16), pl.ds(d * bunch_dev, bunch_dev)] = high
                low_ref[pl.ds(at, 16), pl.ds(d * bunch_dev, bunch_dev)] = low
        return carry

    for turn in range(turns):
        circulant(turn, 0)
    copies[2].wait()
    copies[3].wait()
    digit = lax.broadcasted_iota(jnp.int32, (16, 128), 0)
    octal = lax.broadcasted_iota(jnp.int32, (8, 128), 0)

    owner = lax.broadcasted_iota(jnp.int32, (16, 128), 1) >> 4

    def deposit(group, carry):
        lows, values = [], []
        for inner in range(8):
            bunch = group * 8 + inner
            low_rows, value_rows = [], []
            for chunk in range(chunks):
                place = index_ref[pl.ds(bunch * chunks + chunk, 1), :]
                low_rows.append(jnp.where(digit == (place & 15), 1.0, 0.0))
                hit = octal == (place >> 4)
                base = (bunch * chunks + chunk) * 4
                value_rows.append(jnp.concatenate([
                    jnp.where(hit, coord_ref[pl.ds(base + 2 * plane, 1), :], 0.0) for plane in range(2)
                ], 0))
            lows.append(jnp.concatenate(low_rows, 1).astype(jnp.bfloat16))
            values.append(jnp.concatenate(value_rows, 1))
        both = jnp.concatenate(split(jnp.concatenate(values, 0)), 0)
        out = lax.dot_general(
            both, jnp.concatenate(lows, 0), (((1,), (1,)), ((), ())), preferred_element_type=jnp.float32
        )
        placed = jnp.zeros((16, 128), jnp.float32)
        for inner in range(8):
            at = 16 * inner
            placed = jnp.where(owner == inner, out[at : at + 16] + out[128 + at : 144 + at], placed)
        at = pl.ds(pl.multiple_of(group * 8, 8), 8)
        group_ref[0, at, :] = placed[:8]
        group_ref[1, at, :] = placed[8:]
        return carry

    lax.fori_loop(0, bunch_dev // 8, deposit, 0, unroll=16)
    lanes16 = lax.broadcasted_iota(jnp.int32, (16, 128), 1)
    for plane in range(2):
        turned = group_ref[plane].T
        blocks = swap_bits([turned[16 * i : 16 * i + 16] for i in range(8)], lanes16)
        current = jnp.concatenate(blocks, 0) * (slices / (chunks * 128))
        moments_ref[plane] = current
        high, low = ((now_high_ref, now_low_ref), (later_high_ref, later_low_ref))[plane]
        high[:, :bunch_dev], low[:, :bunch_dev] = split(current)

    moment_copy = pltpu.make_async_copy(moments_ref, moments_hbm, sems.at[5])
    moment_copy.start()
    copies[4].wait()

    def spread(turn, carry):
        at = pl.ds(pl.multiple_of(turn * bunch_dev, bunch_dev), bunch_dev)
        now_high_ref[:, at], now_low_ref[:, at] = split(history_ref[turn - 1, :slices])
        later_high_ref[:, at], later_low_ref[:, at] = split(history_ref[turn - 1, slices:])
        return carry

    for turn in range(1, turns):
        spread(turn, 0)

    reach(place_ref[0], (now_high_ref, now_low_ref), (high_ref, low_ref), keep_ref, send_ref)
    moment_copy.wait()


def track_kernel(plane, coef_ref, coord_ref, index_ref, wake_ref, part_refs, kick_ref, store, finish):
    bunch_dev = wake_ref.shape[0]
    chunks = index_ref.shape[0] // bunch_dev
    field = part_refs[0][...]
    for ref in part_refs[1:]:
        field = field + ref[...]
    kick_ref[...] = wide_dot(split(field.T), split(wake_ref[...].T))
    tune, detune = coef_ref[plane], coef_ref[2 + plane]

    def group(step, carry):
        table = kick_ref[pl.ds(pl.multiple_of(step * 8, 8), 8), :]
        for chunk in range(chunks):
            picked = index_ref[pl.ds(step * 8 * chunks + chunk, 8, stride=chunks), :]
            start = step * 32 * chunks + 4 * chunk + 2 * plane
            push = jnp.take_along_axis(table, picked, axis=1)
            position = coord_ref[pl.ds(start, 8, stride=4 * chunks), :]
            slope = coord_ref[pl.ds(start + 1, 8, stride=4 * chunks), :] + push
            square = position * position + slope * slope
            cosine, sine = rotation(tune + detune * square)
            store(step, chunk, cosine * position + sine * slope, cosine * slope - sine * position)
        return carry

    steps = bunch_dev // 8
    for piece in range(4):
        lax.fori_loop(piece * steps // 4, (piece + 1) * steps // 4, group, 0, unroll=4)
        finish(piece)


def first_kernel(coef_ref, coord_ref, index_ref, wake_ref, *rest):
    part_refs, (moved_ref, kick_ref) = rest[:-2], rest[-2:]
    chunks = index_ref.shape[0] // wake_ref.shape[0]

    def store(step, chunk, position, slope):
        at = pl.ds(step * 8 * chunks + chunk, 8, stride=chunks)
        moved_ref[0, at, :] = position
        moved_ref[1, at, :] = slope

    track_kernel(0, coef_ref, coord_ref, index_ref, wake_ref, part_refs, kick_ref, store, lambda piece: None)


def second_kernel(coef_ref, coord_ref, index_ref, wake_ref, first_ref, *rest):
    part_refs, (moved_hbm, kick_ref, moved_ref, sems) = rest[:-4], rest[-4:]
    bunch_dev = wake_ref.shape[0]
    chunks = index_ref.shape[0] // bunch_dev
    copies = []

    def store(step, chunk, position, slope):
        start = step * 32 * chunks + 4 * chunk
        source = pl.ds(step * 8 * chunks + chunk, 8, stride=chunks)
        moved = (first_ref[0, source, :], first_ref[1, source, :], position, slope)
        for i in range(4):
            moved_ref[pl.ds(start + i, 8, stride=4 * chunks), :] = moved[i]

    def finish(piece):
        span = pl.ds(piece * bunch_dev * chunks, bunch_dev * chunks)
        copies.append(pltpu.make_async_copy(moved_ref.at[span], moved_hbm.at[span], sems.at[piece]))
        copies[-1].start()

    track_kernel(1, coef_ref, coord_ref, index_ref, wake_ref, part_refs, kick_ref, store, finish)
    for copy in copies:
        copy.wait()


def hop_order(half):
    return [*range(max(1, half // 2), half), *range(1, half // 2)]


def staged(coordinates, slice_index, history, impedance, slice_wake, tunes, detuning):
    turn_total, _, slice_count, bunch_dev = history.shape
    trains = lax.axis_size("train")
    bunch_total = trains * bunch_dev
    half = trains // 2
    lanes = 128
    columns = slice_index.shape[0] // lanes
    grid = coordinates.reshape(4, columns, lanes).transpose(1, 0, 2).reshape(4 * columns, lanes)
    picked = slice_index.reshape(columns, lanes)
    stacked = history.reshape(turn_total, 2 * slice_count, bunch_dev)
    rows = impedance.reshape(turn_total + 1, 2, trains, bunch_dev).transpose(0, 2, 1, 3)
    rows = rows.reshape((turn_total + 1) * 2 * trains, bunch_dev)
    fine = wave_table(trains, bunch_dev)
    place = lax.axis_index("train").reshape(1)
    vmem = pl.BlockSpec(memory_space=pltpu.VMEM)
    smem = pl.BlockSpec(memory_space=pltpu.SMEM)
    hbm = pl.BlockSpec(memory_space=pltpu.HBM)
    block = jax.ShapeDtypeStruct((half, slice_count, bunch_dev), jnp.float32)
    depth = (turn_total + 1) * bunch_dev
    matrix = jax.ShapeDtypeStruct((depth, bunch_total), jnp.bfloat16)
    series = jax.ShapeDtypeStruct((slice_count, depth), jnp.bfloat16)
    moments, keep0, send0, *later = pl.pallas_call(
        front_kernel,
        out_shape=(
            jax.ShapeDtypeStruct((2, slice_count, bunch_dev), jnp.float32),
            block, block, matrix, matrix, series, series,
        ),
        in_specs=[smem] + [hbm] * 5,
        out_specs=[hbm] + [vmem] * 6,
        scratch_shapes=[
            pltpu.VMEM((2, slice_count, bunch_dev), jnp.float32),
            pltpu.VMEM(series.shape, jnp.bfloat16),
            pltpu.VMEM(series.shape, jnp.bfloat16),
            pltpu.VMEM(grid.shape, jnp.float32),
            pltpu.VMEM(picked.shape, jnp.int32),
            pltpu.VMEM(stacked.shape, jnp.float32),
            pltpu.VMEM((2, bunch_dev, slice_count), jnp.float32),
            pltpu.VMEM((rows.shape[0], 2 * bunch_total), jnp.float32),
            pltpu.VMEM(rows.shape, jnp.float32),
            pltpu.VMEM(fine.shape, jnp.bfloat16),
            pltpu.SemaphoreType.DMA((6,)),
        ],
        compiler_params=pltpu.CompilerParams(vmem_limit_bytes=32 * 2**20),
        name="front",
    )(place, *[pltpu.with_memory_space_constraint(x, pltpu.HBM) for x in (grid, picked, stacked, rows, fine)])

    keep1, send1 = pl.pallas_call(
        back_kernel,
        out_shape=(block, block),
        in_specs=[smem] + [vmem] * 4,
        out_specs=[vmem] * 2,
        compiler_params=pltpu.CompilerParams(vmem_limit_bytes=16 * 2**20),
        cost_estimate=pl.CostEstimate(flops=2 * 10**9, transcendentals=0, bytes_accessed=10**6),
        name="back",
    )(place, *later)

    pairs = [(i, i ^ 1) for i in range(trains)]
    parts = []
    for keep, send in ((keep0, send0), (keep1, send1)):
        far = lax.ppermute(send, "train", pairs)
        near = [keep[hop] + far[hop] for hop in range(half)]
        mine = [near[0]]
        for hop in hop_order(half)[::-1]:
            mine.append(lax.ppermute(near[hop], "train", [(i, i ^ (2 * hop)) for i in range(trains)]))
        parts.append(mine)
    marked = lax.optimization_barrier((tunes, detuning, parts[0][1]))
    coefs = jnp.concatenate([marked[0] * 4.0, marked[1] * (1.0 / math.pi)])
    parts[0][1] = marked[2]

    estimate = pl.CostEstimate(flops=2 * 10**9, transcendentals=0, bytes_accessed=10**6)
    first = pl.pallas_call(
        first_kernel,
        out_shape=jax.ShapeDtypeStruct((2,) + picked.shape, jnp.float32),
        in_specs=[smem] + [vmem] * (3 + half),
        out_specs=vmem,
        scratch_shapes=[pltpu.VMEM((bunch_dev, slice_count), jnp.float32)],
        compiler_params=pltpu.CompilerParams(vmem_limit_bytes=16 * 2**20),
        cost_estimate=estimate,
        name="first",
    )(coefs, grid, picked, slice_wake, *parts[0])
    moved = pl.pallas_call(
        second_kernel,
        out_shape=jax.ShapeDtypeStruct(grid.shape, jnp.float32),
        in_specs=[smem] + [vmem] * (4 + half),
        out_specs=hbm,
        scratch_shapes=[
            pltpu.VMEM((bunch_dev, slice_count), jnp.float32),
            pltpu.VMEM(grid.shape, jnp.float32),
            pltpu.SemaphoreType.DMA((4,)),
        ],
        compiler_params=pltpu.CompilerParams(vmem_limit_bytes=16 * 2**20),
        cost_estimate=estimate,
        name="second",
    )(coefs, grid, picked, slice_wake, first, *parts[1])
    tracked = moved.reshape(columns, 4, lanes).transpose(1, 0, 2).reshape(4, columns * lanes)
    return (tracked, moments)


def local(coordinates, slice_index, history, impedance, slice_wake, tunes, detuning):
    trains = lax.axis_size("train")
    slice_count, bunch_dev = history.shape[2:]
    per_bunch = slice_index.shape[0] // bunch_dev
    fits = slice_count == bunch_dev == 128 and per_bunch % 128 == 0 and trains in (2, 4, 8, 16)
    body = staged if fits else generic
    return body(coordinates, slice_index, history, impedance, slice_wake, tunes, detuning)


def solution(mesh):
    return jax.shard_map(
        local,
        mesh=mesh,
        in_specs=(
            P("seed", "train"),
            P(("seed", "train")),
            P("seed", None, None, "train"),
            P(),
            P(),
            P("seed"),
            P("seed"),
        ),
        out_specs=(P("seed", "train"), P("seed", None, "train")),
        check_vma=False,
    )
```
